32 devices in a mesh: row: 8 (over z, y), col: 4 (over x, core).
Axes of the slice: x: 2, y: 2, z: 4, core: 2. Of those that a mesh axis runs over, the one named last changes fastest.
Arguments:
- tile_values: bfloat16 [128, 8, 256, 256], P(('row', 'col')), may hold values from -0.375 to 0.375
- block_columns: int32 [128, 8], P(('row', 'col')), may hold values from 0 to 127, as said below
- tile_counts: int32 [128], P(('row', 'col')), may hold values from 1 to 8, as said below
- diagonal: float32 [32768], P(('row', 'col')), may hold values from 0.5 to 4
- sketch_rows: int32 [32768], P(('row', 'col')), may hold values from 0 to 1023
- sketch_signs: int32 [32768], P(('row', 'col')), may hold values from 0 to 1
- right_side: float32 [16, 32768], P(None, ('row', 'col')), may hold values from -70 to 70
Outputs:
- solution: float32 [16, 32768], P(None, ('row', 'col'))
- last_basis: float32 [16, 32768], P(None, ('row', 'col'))
- hessenberg: float32 [16, 5, 4], replicated
The draws below stay inside these ranges and needn't reach their ends.
Inputs may be any that keep to these rules, and one draw needn't show every extreme that they name: `block_columns`: for block row b all 8 entries are distinct block columns c with (c - b) mod 128 <= 4 or >= 124; only slots k < tile_counts[b] are used. `tile_counts`: in every draw the 4 block rows of at least one device all have 8.
All inputs are finite; a program needn't handle non-finite values.
Results may differ from the reference program's by a relative error of at most 0.0053.
Values may be sent and summed in bfloat16 or wider, within the bound.
A program may use at most 64 MiB of HBM per device.

```python
import math
import jax
import jax.numpy as jnp
from jax import lax

TILE = 256
SKETCH = 1024
KMAX = 8
ITERS = 4
BR_DEV = 4
RHS = 16
NB = 128
N = 32768


def draw_block_columns(key, part):
    span = 2 * BR_DEV + 1
    scores = jax.random.randint(jax.random.fold_in(key, 11), (NB, span), 0, 1 << 20) * span + jnp.arange(span)[None, :]
    order = jnp.argsort(scores, axis=1, stable=True)
    offsets = order[:, :KMAX] - BR_DEV
    return ((jnp.arange(NB)[:, None] + offsets) % NB).astype(jnp.int32)


def draw_tile_counts(key, part):
    groups = NB // BR_DEV
    heavy = jax.random.randint(jax.random.fold_in(key, 21), (groups,), 0, 4) == 0
    forced = jnp.arange(groups) == jax.random.randint(jax.random.fold_in(key, 22), (), 0, groups)
    heavy = jnp.logical_or(heavy, forced)
    light = jax.random.randint(jax.random.fold_in(key, 23), (NB,), 1, KMAX // 2 + 1)
    return jnp.where(jnp.repeat(heavy, BR_DEV), KMAX, light).astype(jnp.int32)


def draw_right_side(key, part):
    scales = jnp.exp(jax.random.uniform(jax.random.fold_in(key, 31), (1, NB, 1), minval=0.0, maxval=math.log(10.0)))
    value = jax.random.truncated_normal(jax.random.fold_in(key, 32), -6.0, 6.0, (RHS, NB, TILE)) * scales
    return value.reshape(RHS, NB * TILE).astype(jnp.float32)


def with_ends(values, key, least, high):
    extent = values.shape
    index_at = [jax.random.randint(jax.random.fold_in(key, axis), (), 0, extent[axis]) for axis in range(len(extent))]
    values = values.at[tuple(index_at)].set(least)
    longest = extent.index(max(extent))
    index_at[longest] = (index_at[longest] + 1) % extent[longest]
    return values.at[tuple(index_at)].set(high)


def block_scale(rng, dims, pieces, low, high):
    level = 1.0
    for position, parts in pieces:
        draws = jax.random.uniform(jax.random.fold_in(jax.random.fold_in(rng, 6), position), (parts,), jnp.float32, low / len(pieces), high / len(pieces))
        level = level * jnp.repeat(jnp.exp(draws), dims[position] // parts).reshape((-1,) + (1,) * (len(dims) - 1 - position))
    return level


def noise(own_key, extent, spread, most, shards=(), dtype=jnp.bfloat16):
    values = spread * jax.random.normal(own_key, extent, jnp.float32)
    if shards:
        values = values * block_scale(own_key, extent, shards, -0.22, 0.18)
    return jnp.clip(values, -most, most).astype(dtype)


def setup_inputs(seed: int = 0) -> dict:
    key_of = jax.random.split(jax.random.key(seed), 8)
    return {
        "tile_values": noise(key_of[0], (NB, KMAX, TILE, TILE), TILE ** -0.5, 0.375, ((0, 32),)),
        "block_columns": draw_block_columns(jax.random.fold_in(key_of[7], 71), 0),
        "tile_counts": draw_tile_counts(jax.random.fold_in(key_of[7], 71), 0),
        "diagonal": jnp.clip(jnp.exp(math.log(4.0) - 2.0794415 * jax.random.uniform(key_of[3], (N,), jnp.float32) ** block_scale(key_of[3], (N,), ((0, 32),), -0.2, 0.2)), 0.5, 4.0),
        "sketch_rows": with_ends(jax.random.randint(key_of[4], (N,), 0, SKETCH), jax.random.fold_in(key_of[4], 1), 0, SKETCH - 1).astype(jnp.int32),
        "sketch_signs": with_ends(jax.random.randint(key_of[5], (N,), 0, 2), jax.random.fold_in(key_of[5], 1), 0, 1).astype(jnp.int32),
        "right_side": draw_right_side(jax.random.fold_in(key_of[7], 71), 0),
    }


epsilon = 1e-06
highest = lax.Precision.HIGHEST

def cholesky_solve(gram, target):
    order = gram.shape[1]
    factor = {}
    for column in range(order):
        diag_part = gram[:, column, column]
        for inner in range(column):
            diag_part = diag_part - factor[column, inner] * factor[column, inner]
        factor[column, column] = jnp.sqrt(diag_part)
        for below in range(column + 1, order):
            entry = gram[:, below, column]
            for inner in range(column):
                entry = entry - factor[below, inner] * factor[column, inner]
            factor[below, column] = entry / factor[column, column]
    forward = []
    for column in range(order):
        entry = target[:, column]
        for inner in range(column):
            entry = entry - factor[column, inner] * forward[inner]
        forward.append(entry / factor[column, column])
    result = [None] * order
    for column in reversed(range(order)):
        entry = forward[column]
        for inner in range(column + 1, order):
            entry = entry - factor[inner, column] * result[inner]
        result[column] = entry / factor[column, column]
    return jnp.stack(result, axis=1)

def sketch_solve(stacked, image_sketch):
    gram = jnp.einsum('rjk,rmk->rjm', stacked, stacked, precision=highest)
    target = jnp.einsum('rjk,rk->rj', stacked, image_sketch, precision=highest)
    return cholesky_solve(gram, target)

def sketch_of(vector, sketch_rows, sketch_signs):
    signed = vector * (2 * sketch_signs - 1).astype(jnp.float32)[None, :]
    summed = jax.ops.segment_sum(signed.T, sketch_rows, num_segments=SKETCH)
    return summed.T / math.sqrt(N)

def apply_matrix(vector, tile_values, block_columns, tile_counts, diagonal):
    blocks = vector.astype(jnp.bfloat16).reshape(RHS, NB, TILE)
    live_mask = (jnp.arange(KMAX)[None, :] < tile_counts[:, None]).astype(jnp.float32)

    def add_slot(slot_turn, running):
        slot_tiles = lax.dynamic_index_in_dim(tile_values, slot_turn, 1, keepdims=False).astype(jnp.float32)
        wanted = lax.dynamic_index_in_dim(block_columns, slot_turn, 1, keepdims=False)
        picked = jnp.take(blocks, wanted, axis=1).astype(jnp.float32)
        weight_mask = lax.dynamic_index_in_dim(live_mask, slot_turn, 1, keepdims=False)
        product = jnp.einsum('rbi,boi->rbo', picked, slot_tiles, precision=highest)
        return running + product * weight_mask[None, :, None]
    tile_sum = lax.fori_loop(0, KMAX, add_slot, jnp.zeros((RHS, NB, TILE), jnp.float32))
    return diagonal[None, :] * vector + tile_sum.reshape(RHS, N)

def reference(tile_values, block_columns, tile_counts, diagonal, sketch_rows, sketch_signs, right_side):
    start = sketch_of(right_side, sketch_rows, sketch_signs)
    beta = jnp.sqrt(lax.optimization_barrier(jnp.sum(start * start, axis=1)) + epsilon)
    basis = [right_side / beta[:, None]]
    sketched = [start / beta[:, None]]
    columns_list = []
    for step_index in range(ITERS):
        image = apply_matrix(basis[-1], tile_values, block_columns, tile_counts, diagonal)
        image_sketch = sketch_of(image, sketch_rows, sketch_signs)
        stacked = jnp.stack(sketched, axis=1)
        coeffs = sketch_solve(stacked, image_sketch)
        fresh = image - jnp.einsum('rj,rjn->rn', coeffs, jnp.stack(basis, axis=1), precision=highest)
        fresh_sketch = sketch_of(fresh, sketch_rows, sketch_signs)
        norm_new = jnp.sqrt(lax.optimization_barrier(jnp.sum(fresh_sketch * fresh_sketch, axis=1)) + epsilon)
        basis.append(fresh / norm_new[:, None])
        sketched.append(fresh_sketch / norm_new[:, None])
        padding = jnp.zeros((RHS, ITERS - step_index - 1), jnp.float32)
        columns_list.append(jnp.concatenate([coeffs, norm_new[:, None], padding], axis=1))
    hessenberg = jnp.stack(columns_list, axis=2)
    gram = jnp.einsum('rim,rin->rmn', hessenberg, hessenberg, precision=highest)
    weights = cholesky_solve(gram, beta[:, None] * hessenberg[:, 0, :])
    solution = jnp.einsum('rm,rmn->rn', weights, jnp.stack(basis[:ITERS], axis=1), precision=highest)
    return (solution, basis[-1], hessenberg)
```

```python
import functools
import math

import jax
import jax.numpy as jnp
from jax import lax
from jax.experimental import pallas as pl
from jax.experimental.pallas import tpu as pltpu
from jax.sharding import PartitionSpec as P

SKETCH = 1024
ITERS = 4
SHIFT = 1.75
epsilon = 1e-06
MESH = pl.DeviceIdType.MESH
f32 = jnp.float32
bf16 = jnp.bfloat16


def split_parts(value):
    head = value.astype(bf16)
    return jnp.concatenate([head, (value - head.astype(f32)).astype(bf16)], axis=0)


def extend_factor(factor, inverse, entries):
    row = len(inverse)
    for column in range(row):
        entry = entries[column]
        for inner in range(column):
            entry = entry - factor[row, inner] * factor[column, inner]
        factor[row, column] = entry * inverse[column]
    diag_part = entries[row]
    for inner in range(row):
        diag_part = diag_part - factor[row, inner] * factor[row, inner]
    inverse.append(lax.rsqrt(diag_part))


def factor_solve(factor, inverse, target):
    order = len(target)
    forward = []
    for column in range(order):
        entry = target[column]
        for inner in range(column):
            entry = entry - factor[column, inner] * forward[inner]
        forward.append(entry * inverse[column])
    result = [None] * order
    for column in reversed(range(order)):
        entry = forward[column]
        for inner in range(column + 1, order):
            entry = entry - factor[inner, column] * result[inner]
        result[column] = entry * inverse[column]
    return result


def nn_dot(a, b):
    return lax.dot_general(a, b, (((1,), (0,)), ((), ())), preferred_element_type=f32)


def kernel(
    rows,
    cols,
    scaling,
    columns_hbm,
    counts_hbm,
    diag_hbm,
    rows_hbm,
    signs_hbm,
    right_hbm,
    tiles_hbm,
    solution_ref,
    last_ref,
    hess_ref,
    columns_ref,
    counts_ref,
    diag_ref,
    rows_ref,
    signs_ref,
    tiles,
    band,
    index_ref,
    projector,
    krylov,
    window,
    part,
    land1,
    land2,
    grams,
    load_sem,
    tile_sem,
    halo_send,
    halo_recv,
    send1,
    recv1,
    send2,
    recv2,
    send3,
    recv3,
):
    row = lax.axis_index("row")
    col = lax.axis_index("col")
    devices = rows * cols
    me = row * cols + col
    block_rows, slots, tile, _ = tiles_hbm.shape
    span = 2 * block_rows + 1
    systems, width = right_hbm.shape
    all_blocks = block_rows * devices
    share = SKETCH // cols
    right = lax.rem(me + 1, devices)
    left = lax.rem(me + devices - 1, devices)
    right = (lax.div(right, cols), lax.rem(right, cols))
    left = (lax.div(left, cols), lax.rem(left, cols))
    col_to = [lax.rem(col + off, cols) for off in range(cols)]
    col_from = [lax.rem(col + cols - off, cols) for off in range(cols)]
    row_to = [lax.rem(row + off, rows) for off in range(rows)]
    row_from = [lax.rem(row + rows - off, rows) for off in range(rows)]

    barrier = pltpu.get_barrier_semaphore()
    for peer in (left, right):
        pl.semaphore_signal(barrier, inc=1, device_id=peer, device_id_type=MESH)
    for off in range(1, rows):
        pl.semaphore_signal(barrier, inc=1, device_id=(row_to[off], col), device_id_type=MESH)
    for off in range(1, cols):
        pl.semaphore_signal(barrier, inc=1, device_id=(row, col_to[off]), device_id_type=MESH)

    loads = [
        pltpu.make_async_copy(source, target, load_sem.at[n])
        for n, (source, target) in enumerate(
            [
                (rows_hbm, rows_ref),
                (signs_hbm, signs_ref),
                (columns_hbm, columns_ref),
                (counts_hbm, counts_ref),
                (diag_hbm, diag_ref),
            ]
            + [
                (right_hbm.at[:, pl.ds(b * tile, tile)], krylov.at[0, b])
                for b in range(block_rows)
            ]
        )
    ]
    tile_loads = [
        pltpu.make_async_copy(tiles_hbm.at[b], tiles.at[pl.ds(b * slots, slots)], tile_sem.at[b])
        for b in range(block_rows)
    ]
    for load in loads + tile_loads:
        load.start()
    tiles[block_rows * slots] = jnp.zeros((tile, tile), bf16)

    def halo_copies(k, b):
        return [
            pltpu.make_async_remote_copy(
                src_ref=window.at[k, block_rows + b],
                dst_ref=window.at[k, 2 * side * block_rows + b],
                send_sem=halo_send.at[k, side, b],
                recv_sem=halo_recv.at[k, side, b],
                device_id=peer,
                device_id_type=MESH,
            )
            for side, peer in ((0, right), (1, left))
        ]

    def copy1(k, off, block):
        return pltpu.make_async_remote_copy(
            src_ref=part.at[k, block],
            dst_ref=land1.at[k, off - 1],
            send_sem=send1.at[k, off - 1],
            recv_sem=recv1.at[k, off - 1],
            device_id=(row, col_to[off]),
            device_id_type=MESH,
        )

    def copy2(k, off, source):
        return pltpu.make_async_remote_copy(
            src_ref=land2.at[k, source],
            dst_ref=land2.at[k, source],
            send_sem=send2.at[k, off - 1],
            recv_sem=recv2.at[k, off - 1],
            device_id=(row_to[off], col),
            device_id_type=MESH,
        )

    def copy3(g, off, source):
        return pltpu.make_async_remote_copy(
            src_ref=grams.at[g, source],
            dst_ref=grams.at[g, source],
            send_sem=send3.at[g, off - 1],
            recv_sem=recv3.at[g, off - 1],
            device_id=(row, col_to[off]),
            device_id_type=MESH,
        )

    for load in loads[4:]:
        load.wait()
    for b in range(block_rows):
        window[0, block_rows + b] = split_parts(krylov[0, b])
    pl.semaphore_wait(barrier, rows + cols)
    for b in range(block_rows):
        for copy in halo_copies(0, b):
            copy.start()

    for load in loads[:4]:
        load.wait()
    first = me * block_rows
    for b in range(block_rows):
        spots = []
        for slot in range(slots):
            spot = lax.rem(columns_ref[b, slot] - first - b + block_rows + all_blocks, all_blocks)
            spots.append(jnp.where(slot < counts_ref[b], spot, span))
        for d in range(span):
            chosen = block_rows * slots
            for slot in range(slots):
                chosen = jnp.where(spots[slot] == d, b * slots + slot, chosen)
            index_ref[b * span + d] = chosen

    lanes = 128
    for c in range(width // lanes):
        here = pl.ds(c * lanes, lanes)
        target = jnp.broadcast_to(rows_ref[0:1, here].astype(f32), (lanes, lanes)).T
        sign = jnp.broadcast_to((2 * signs_ref[0:1, here] - 1).astype(f32), (lanes, lanes)).T
        for m in range(SKETCH // lanes):
            spot = (lax.broadcasted_iota(jnp.int32, (lanes, lanes), 1) + m * lanes).astype(f32)
            projector[here, pl.ds(m * lanes, lanes)] = jnp.where(spot == target, sign, 0.0).astype(bf16)

    for load in tile_loads:
        load.wait()

    def turn(i, carry):
        band[i] = tiles[index_ref[i]].T
        return carry

    lax.fori_loop(0, block_rows * span, turn, 0)

    def fold(total):
        return total[:systems] + total[systems:]

    def matvec(k, b, spots):
        total = None
        for spot in spots:
            if 0 <= spot - b < span:
                term = nn_dot(window[k, spot], band[b * span + spot - b])
                total = term if total is None else total + term
        return fold(total)

    own = list(range(block_rows, 2 * block_rows))
    outer = list(range(block_rows)) + list(range(2 * block_rows, 3 * block_rows))

    def stage1(k, values):
        for block in range(cols):
            total = None
            for b in range(block_rows):
                term = nn_dot(
                    values[b], projector[pl.ds(b * tile, tile), pl.ds(block * share, share)]
                )
                total = term if total is None else total + term
            part[k, block] = fold(total) * scaling
        for off in range(1, cols):
            copy1(k, off, col_to[off]).start()

    def stage2(k):
        for off in range(1, cols):
            copy1(k, off, 0).wait_recv()
        total = part[k, col]
        for off in range(1, cols):
            total = total + land1[k, off - 1]
        land2[k, row] = total
        for off in range(1, rows):
            copy2(k, off, row).start()

    def gathered(k):
        for off in range(1, rows):
            copy2(k, off, row_from[off]).wait_recv()
        total = land2[k, 0]
        for r in range(1, rows):
            total = total + land2[k, r]
        return total

    for k in range(ITERS):
        for b in range(block_rows):
            diag_b = diag_ref[0:1, pl.ds(b * tile, tile)] - SHIFT
            krylov[k + 1, b] = diag_b * krylov[k, b] + matvec(k, b, own)
        stage1(k, [window[k, block_rows + b] for b in range(block_rows)])
        if k >= 1:
            stage2(k - 1)
        for b in range(block_rows):
            for copy in halo_copies(k, b):
                copy.wait_recv()
        values = []
        for b in range(block_rows):
            fresh = krylov[k + 1, b] + matvec(k, b, outer)
            krylov[k + 1, b] = fresh
            values.append(split_parts(fresh))
            if k + 1 < ITERS:
                window[k + 1, block_rows + b] = values[b]
                for copy in halo_copies(k + 1, b):
                    copy.start()
    stage1(ITERS, values)
    stage2(ITERS - 1)

    lane = lax.broadcasted_iota(jnp.int32, (systems, lanes), 1)
    sketches = []

    def pair_sums(pairs):
        packed = jnp.zeros((systems, lanes), f32)
        for p, (i, j) in enumerate(pairs):
            value = jnp.sum(sketches[i] * sketches[j], axis=1, keepdims=True)
            packed = jnp.where(lane == p, value, packed)
        return packed

    def publish(g, packed):
        grams[g, col] = packed
        for off in range(1, cols):
            copy3(g, off, col).start()

    def collect(g, pairs, gram):
        for off in range(1, cols):
            copy3(g, off, col_from[off]).wait_recv()
        total = grams[g, 0]
        for c in range(1, cols):
            total = total + grams[g, c]
        for p, pair in enumerate(pairs):
            gram[pair] = jnp.broadcast_to(total[:, p : p + 1], (systems, lanes))

    early = [(i, j) for i in range(ITERS) for j in range(i + 1)]
    late = [(ITERS, j) for j in range(ITERS + 1)]
    for k in range(ITERS - 1):
        sketches.append(gathered(k))
    stage2(ITERS)
    sketches.append(gathered(ITERS - 1))
    publish(0, pair_sums(early))
    sketches.append(gathered(ITERS))
    publish(1, pair_sums(late))

    gram = {}
    lower = {}
    upright = []
    coords = []
    lengths = []
    hess = {}
    normal, normal_inverse = {}, []

    def lower_row(i):
        for j in range(i + 1):
            entry = gram[i, j]
            for m in range(j):
                entry = entry - lower[i, m] * lower[j, m]
            if j < i:
                lower[i, j] = entry * upright[j]
            else:
                upright.append(lax.rsqrt(entry))
                lower[i, i] = entry * upright[i]

    def arnoldi(j):
        image = [SHIFT * entry for entry in coords[j - 1]] + [coords[j - 1][j - 1]]
        for m in range(1, j):
            image[m] = image[m] + coords[j - 1][m - 1]
        fresh = image
        for i in range(j):
            seen = image[i] * lower[i, i]
            for m in range(i + 1, j + 1):
                seen = seen + image[m] * lower[m, i]
            coeff = seen * lengths[i]
            hess[i, j - 1] = coeff
            fresh = [
                entry - coeff * coords[i][m] if m <= i else entry for m, entry in enumerate(fresh)
            ]
        length = image[j] * lower[j, j]
        square = length * length + epsilon
        scale = lax.rsqrt(square)
        hess[j, j - 1] = square * scale
        coords.append([entry * scale for entry in fresh])
        lengths.append(1.0 / (length * scale))
        entries = []
        for n in range(j):
            entry = None
            for i in range(n + 2):
                term = hess[i, j - 1] * hess[i, n]
                entry = term if entry is None else entry + term
            entries.append(entry)
        extend_factor(normal, normal_inverse, entries)

    collect(0, early, gram)
    for i in range(ITERS):
        lower_row(i)
    square = gram[0, 0] + epsilon
    scale = lax.rsqrt(square)
    beta = square * scale
    coords.append([scale])
    lengths.append(1.0 / (lower[0, 0] * scale))
    for j in range(1, ITERS):
        arnoldi(j)
    collect(1, late, gram)
    lower_row(ITERS)
    arnoldi(ITERS)

    packed = jnp.zeros((systems, lanes), f32)
    for (i, j), value in hess.items():
        packed = jnp.where(lane == i * ITERS + j, value, packed)
    turned = packed.T
    for i in range(ITERS + 1):
        hess_ref[i] = turned[i * ITERS : (i + 1) * ITERS, :]

    weights = factor_solve(normal, normal_inverse, [beta * hess[0, n] for n in range(ITERS)])
    mixed = []
    for m in range(ITERS):
        entry = None
        for i in range(m, ITERS):
            term = weights[i] * coords[i][m]
            entry = term if entry is None else entry + term
        mixed.append(entry)

    def combine(target, factors, b):
        for c in range(tile // lanes):
            out = None
            for m, factor in enumerate(factors):
                term = factor * krylov[m, b, :, pl.ds(c * lanes, lanes)]
                out = term if out is None else out + term
            target[:, pl.ds(b * tile + c * lanes, lanes)] = out

    for b in range(block_rows):
        combine(last_ref, coords[ITERS], b)
        combine(solution_ref, mixed, b)

    for k in range(ITERS + 1):
        if k < ITERS:
            for b in range(block_rows):
                for copy in halo_copies(k, b):
                    copy.wait_send()
        for off in range(1, cols):
            copy1(k, off, col_to[off]).wait_send()
        for off in range(1, rows):
            copy2(k, off, row).wait_send()
    for g in range(2):
        for off in range(1, cols):
            copy3(g, off, col).wait_send()


def local(
    rows, cols, tile_values, block_columns, tile_counts, diagonal, sketch_rows, sketch_signs, right_side
):
    block_rows, slots, tile, _ = tile_values.shape
    span = 2 * block_rows + 1
    systems, width = right_side.shape
    scaling = 1.0 / math.sqrt(width * rows * cols)
    share = SKETCH // cols
    vectors = ITERS + 1
    vmem = pl.BlockSpec(memory_space=pltpu.VMEM)
    hbm = pl.BlockSpec(memory_space=pltpu.HBM)
    dma = pltpu.SemaphoreType.DMA
    iterate, last, hessenberg = pl.pallas_call(
        functools.partial(kernel, rows, cols, scaling),
        out_shape=(
            pltpu.VMEM((systems, width), f32),
            pltpu.VMEM((systems, width), f32),
            pltpu.VMEM((ITERS + 1, ITERS, systems), f32),
        ),
        in_specs=[hbm] * 7,
        out_specs=(vmem, vmem, vmem),
        scratch_shapes=[
            pltpu.SMEM(block_columns.shape, jnp.int32),
            pltpu.SMEM(tile_counts.shape, jnp.int32),
            pltpu.VMEM((1, width), f32),
            pltpu.VMEM((1, width), jnp.int32),
            pltpu.VMEM((1, width), jnp.int32),
            pltpu.VMEM((block_rows * slots + 1, tile, tile), bf16),
            pltpu.VMEM((block_rows * span, tile, tile), bf16),
            pltpu.SMEM((block_rows * span,), jnp.int32),
            pltpu.VMEM((width, SKETCH), bf16),
            pltpu.VMEM((vectors, block_rows, systems, tile), f32),
            pltpu.VMEM((ITERS, 3 * block_rows, 2 * systems, tile), bf16),
            pltpu.VMEM((vectors, cols, systems, share), f32),
            pltpu.VMEM((vectors, cols - 1, systems, share), f32),
            pltpu.VMEM((vectors, rows, systems, share), f32),
            pltpu.VMEM((2, cols, systems, 128), f32),
            dma((block_rows + 5,)),
            dma((block_rows,)),
            dma((ITERS, 2, block_rows)),
            dma((ITERS, 2, block_rows)),
            dma((vectors, cols - 1)),
            dma((vectors, cols - 1)),
            dma((vectors, rows - 1)),
            dma((vectors, rows - 1)),
            dma((2, cols - 1)),
            dma((2, cols - 1)),
        ],
        compiler_params=pltpu.CompilerParams(
            collective_id=0, has_side_effects=True, vmem_limit_bytes=67043328 - 160 * 1024
        ),
    )(
        block_columns,
        tile_counts,
        diagonal.reshape(1, width),
        sketch_rows.reshape(1, width),
        sketch_signs.reshape(1, width),
        right_side,
        tile_values,
    )
    return iterate, last, jnp.transpose(hessenberg, (2, 0, 1))


def solution(mesh):
    spec = P(("row", "col"))
    in_specs = (
        P(("row", "col"), None, None, None),
        P(("row", "col"), None),
        spec,
        spec,
        spec,
        spec,
        P(None, ("row", "col")),
    )
    out_specs = (P(None, ("row", "col")), P(None, ("row", "col")), P())
    body = functools.partial(local, mesh.shape["row"], mesh.shape["col"])
    return jax.shard_map(body, mesh=mesh, in_specs=in_specs, out_specs=out_specs, check_vma=False)
```

```python
import functools
import math

import jax
import jax.numpy as jnp
from jax import lax
from jax.experimental import pallas as pl
from jax.experimental.pallas import tpu as pltpu
from jax.sharding import PartitionSpec as P

SKETCH = 1024
ITERS = 4
SHIFT = 1.75
epsilon = 1e-06
MESH = pl.DeviceIdType.MESH
f32 = jnp.float32
bf16 = jnp.bfloat16


def split_parts(value):
    head = value.astype(bf16)
    return jnp.concatenate([head, (value - head.astype(f32)).astype(bf16)], axis=0)


def extend_factor(factor, inverse, entries):
    row = len(inverse)
    for column in range(row):
        entry = entries[column]
        for inner in range(column):
            entry = entry - factor[row, inner] * factor[column, inner]
        factor[row, column] = entry * inverse[column]
    diag_part = entries[row]
    for inner in range(row):
        diag_part = diag_part - factor[row, inner] * factor[row, inner]
    inverse.append(lax.rsqrt(diag_part))


def factor_solve(factor, inverse, target):
    order = len(target)
    forward = []
    for column in range(order):
        entry = target[column]
        for inner in range(column):
            entry = entry - factor[column, inner] * forward[inner]
        forward.append(entry * inverse[column])
    result = [None] * order
    for column in reversed(range(order)):
        entry = forward[column]
        for inner in range(column + 1, order):
            entry = entry - factor[inner, column] * result[inner]
        result[column] = entry * inverse[column]
    return result


def nn_dot(a, b):
    return lax.dot_general(a, b, (((1,), (0,)), ((), ())), preferred_element_type=f32)


def kernel(
    rows,
    cols,
    scaling,
    columns_hbm,
    counts_hbm,
    diag_hbm,
    rows_hbm,
    signs_hbm,
    right_hbm,
    tiles_hbm,
    solution_ref,
    last_ref,
    hess_ref,
    columns_ref,
    counts_ref,
    diag_ref,
    rows_ref,
    signs_ref,
    tiles,
    band,
    index_ref,
    projector,
    krylov,
    window,
    part,
    land1,
    land2,
    grams,
    load_sem,
    tile_sem,
    halo_send,
    halo_recv,
    send1,
    recv1,
    send2,
    recv2,
    send3,
    recv3,
):
    row = lax.axis_index("row")
    col = lax.axis_index("col")
    devices = rows * cols
    me = row * cols + col
    block_rows, slots, tile, _ = tiles_hbm.shape
    span = 2 * block_rows + 1
    systems, width = right_hbm.shape
    all_blocks = block_rows * devices
    share = land1.shape[-1]
    team = SKETCH // share
    mates = team // cols
    chains = rows // mates
    right = lax.rem(me + 1, devices)
    left = lax.rem(me + devices - 1, devices)
    right = (lax.div(right, cols), lax.rem(right, cols))
    left = (lax.div(left, cols), lax.rem(left, cols))
    chain = lax.div(row, mates)
    seat = lax.rem(row, mates) * cols + col

    def mate(number):
        return (chain * mates + lax.div(number, cols), lax.rem(number, cols))

    def link(number):
        return (number * mates + lax.rem(row, mates), col)

    parity = lax.rem(seat, 2)
    pair_to = [lax.rem(lax.div(seat, 2) + turn, team // 2) for turn in range(team // 2)]
    sides = [(turn, side) for turn in range(1, team // 2) for side in range(2)] + [(0, 1 - parity)]
    seat_to = [lax.rem(seat + off, team) for off in range(team)]
    seat_from = [lax.rem(seat + team - off, team) for off in range(team)]
    chain_to = [lax.rem(chain + off, chains) for off in range(chains)]
    chain_from = [lax.rem(chain + chains - off, chains) for off in range(chains)]

    right_load = pltpu.make_async_copy(right_hbm, krylov.at[0], load_sem.at[0])
    right_load.start()
    barrier = pltpu.get_barrier_semaphore()
    for peer in (left, right):
        pl.semaphore_signal(barrier, inc=1, device_id=peer, device_id_type=MESH)
    for number in chain_to[1:]:
        pl.semaphore_signal(barrier, inc=1, device_id=link(number), device_id_type=MESH)
    for number in seat_to[1:]:
        pl.semaphore_signal(barrier, inc=1, device_id=mate(number), device_id_type=MESH)

    loads = [
        pltpu.make_async_copy(source, target, load_sem.at[n + 1])
        for n, (source, target) in enumerate(
            [
                (rows_hbm, rows_ref),
                (signs_hbm, signs_ref),
                (columns_hbm, columns_ref),
                (counts_hbm, counts_ref),
                (diag_hbm, diag_ref),
            ]
        )
    ]
    tile_loads = [
        pltpu.make_async_copy(tiles_hbm.at[b], tiles.at[pl.ds(b * slots, slots)], tile_sem.at[b])
        for b in range(block_rows)
    ]
    for load in loads + tile_loads:
        load.start()
    tiles[block_rows * slots] = jnp.zeros((tile, tile), bf16)
    half = block_rows // 2
    lanes = 128

    def block_at(b):
        return pl.ds(b * tile, tile)

    def halo_copies(k, far):
        lower, upper = 0, block_rows - half
        starts = ((0, right, lower if far else upper), (2, left, upper if far else lower))
        return [
            pltpu.make_async_remote_copy(
                src_ref=window.at[k, pl.ds(block_rows + start, half)],
                dst_ref=window.at[k, pl.ds(side * block_rows + start, half)],
                send_sem=halo_send.at[k, side // 2, far],
                recv_sem=halo_recv.at[k, side // 2, far],
                device_id=peer,
                device_id_type=MESH,
            )
            for side, peer, start in starts
        ]

    def send_halo(k):
        for far in range(2):
            for copy in halo_copies(k, far):
                copy.start()

    def copy1(k, turn, side):
        return pltpu.make_async_remote_copy(
            src_ref=part.at[k, 2 * turn + side],
            dst_ref=land1.at[k, 2 * turn + parity],
            send_sem=send1.at[k, 2 * turn + side],
            recv_sem=recv1.at[k, 2 * turn + parity],
            device_id=mate(2 * pair_to[turn] + side),
            device_id_type=MESH,
        )

    def arrival1(k, turn, side):
        return pltpu.make_async_remote_copy(
            src_ref=part.at[k, 2 * turn + side],
            dst_ref=land1.at[k, 2 * turn + side],
            send_sem=send1.at[k, 2 * turn + side],
            recv_sem=recv1.at[k, 2 * turn + side],
            device_id=mate(2 * pair_to[turn] + side),
            device_id_type=MESH,
        )

    def copy2(k, off, source):
        return pltpu.make_async_remote_copy(
            src_ref=land2.at[k, source],
            dst_ref=land2.at[k, source],
            send_sem=send2.at[k, off - 1],
            recv_sem=recv2.at[k, off - 1],
            device_id=link(chain_to[off]),
            device_id_type=MESH,
        )

    def copy3(g, off, source):
        return pltpu.make_async_remote_copy(
            src_ref=grams.at[g, source],
            dst_ref=grams.at[g, source],
            send_sem=send3.at[g, off - 1],
            recv_sem=recv3.at[g, off - 1],
            device_id=mate(seat_to[off]),
            device_id_type=MESH,
        )

    right_load.wait()
    for b in range(block_rows):
        window[0, block_rows + b] = split_parts(krylov[0, :, block_at(b)])
    pl.semaphore_wait(barrier, team + chains)
    send_halo(0)

    for load in loads:
        load.wait()
    first = me * block_rows
    for b in range(block_rows):
        spots = []
        for slot in range(slots):
            spot = lax.rem(columns_ref[b, slot] - first - b + block_rows + all_blocks, all_blocks)
            spots.append(jnp.where(slot < counts_ref[b], spot, span))
        for d in range(span):
            chosen = block_rows * slots
            for slot in range(slots):
                chosen = jnp.where(spots[slot] == d, b * slots + slot, chosen)
            index_ref[b * span + d] = chosen

    for c in range(width // lanes):
        here = pl.ds(c * lanes, lanes)
        target = jnp.broadcast_to(rows_ref[0:1, here].astype(f32), (lanes, lanes)).T
        sign = jnp.broadcast_to((2 * signs_ref[0:1, here] - 1).astype(f32), (lanes, lanes)).T
        for m in range(SKETCH // lanes):
            spot = (lax.broadcasted_iota(jnp.int32, (lanes, lanes), 1) + m * lanes).astype(f32)
            projector[here, pl.ds(m * lanes, lanes)] = jnp.where(spot == target, sign, 0.0).astype(bf16)

    for load in tile_loads:
        load.wait()

    def turn(b, carry):
        for d in range(span):
            band[b * span + d] = tiles[index_ref[b * span + d]].T
        return carry

    lax.fori_loop(0, block_rows, turn, 0)

    def fold(total):
        return total[:systems] + total[systems:]

    def matvec(k, b, spots):
        total = None
        for spot in spots:
            if 0 <= spot - b < span:
                term = nn_dot(window[k, spot], band[b * span + spot - b])
                total = term if total is None else total + term
        return fold(total)

    spots = list(range(3 * block_rows))
    own = spots[block_rows : 2 * block_rows]
    near = spots[half:block_rows] + spots[2 * block_rows : 2 * block_rows + half]
    far = spots[:half] + spots[2 * block_rows + half :]

    def stage1(k, values):
        for turn in list(range(1, team // 2)) + [0]:
            here = pl.ds(pl.multiple_of(pair_to[turn] * 2 * share, 2 * share), 2 * share)
            total = None
            for b in range(block_rows):
                term = nn_dot(values[b], projector[block_at(b), here])
                total = term if total is None else total + term
            total = fold(total) * scaling
            for side in range(2):
                part[k, 2 * turn + side] = total[:, side * share : (side + 1) * share]
            for side in range(2) if turn > 0 else [1 - parity]:
                copy1(k, turn, side).start()

    def stage2(k):
        for turn, side in sides:
            arrival1(k, turn, side).wait_recv()
        total = part[k, parity]
        for turn, side in sides:
            total = total + land1[k, 2 * turn + side]
        land2[k, chain] = total
        for off in range(1, chains):
            copy2(k, off, chain).start()

    def gathered(k):
        for off in range(1, chains):
            copy2(k, off, chain_from[off]).wait_recv()
        total = land2[k, 0]
        for r in range(1, chains):
            total = total + land2[k, r]
        return total

    for k in range(ITERS):
        for b in range(block_rows):
            scaled = (diag_ref[0:1, block_at(b)] - SHIFT) * krylov[k, :, block_at(b)]
            krylov[k + 1, :, block_at(b)] = scaled + matvec(k, b, own)
        for m in range(0 if k == 1 else max(k, 1), k + 1):
            stage1(m, [window[m, block_rows + b] for b in range(block_rows)])
        for m in range(0 if k == 2 else max(k - 1, 1), k):
            stage2(m)
        for copy in halo_copies(k, 0):
            copy.wait_recv()
        for b in range(block_rows):
            krylov[k + 1, :, block_at(b)] += matvec(k, b, near)
        for copy in halo_copies(k, 1):
            copy.wait_recv()
        values = []
        for b in range(block_rows):
            fresh = krylov[k + 1, :, block_at(b)] + matvec(k, b, far)
            krylov[k + 1, :, block_at(b)] = fresh
            values.append(split_parts(fresh))
            if k + 1 < ITERS:
                window[k + 1, block_rows + b] = values[b]
        if k + 1 < ITERS:
            send_halo(k + 1)
    stage1(ITERS, values)
    stage2(ITERS - 1)

    def finish_sends(k):
        for far in range(2 if k < ITERS else 0):
            for copy in halo_copies(k, far):
                copy.wait_send()
        for turn, side in sides:
            copy1(k, turn, side).wait_send()
        for off in range(1, chains):
            copy2(k, off, chain).wait_send()

    lane = lax.broadcasted_iota(jnp.int32, (systems, lanes), 1)
    sketches = []

    def pair_sums(pairs):
        packed = jnp.zeros((systems, lanes), f32)
        for p, (i, j) in enumerate(pairs):
            value = jnp.sum(sketches[i] * sketches[j], axis=1, keepdims=True)
            packed = jnp.where(lane == p, value, packed)
        return packed

    def publish(g, packed):
        grams[g, seat] = packed
        for off in range(1, team):
            copy3(g, off, seat).start()

    def collect(g, pairs, gram):
        for off in range(1, team):
            copy3(g, off, seat_from[off]).wait_recv()
        total = grams[g, 0]
        for c in range(1, team):
            total = total + grams[g, c]
        for p, pair in enumerate(pairs):
            gram[pair] = jnp.broadcast_to(total[:, p : p + 1], (systems, lanes))

    early = [(i, j) for i in range(ITERS) for j in range(i + 1)]
    late = [(ITERS, j) for j in range(ITERS + 1)]
    for k in range(ITERS - 1):
        sketches.append(gathered(k))
    stage2(ITERS)
    sketches.append(gathered(ITERS - 1))
    publish(0, pair_sums(early))
    for k in range(ITERS):
        finish_sends(k)
    sketches.append(gathered(ITERS))
    publish(1, pair_sums(late))

    gram = {}
    lower = {}
    upright = []
    coords = []
    lengths = []
    hess = {}
    normal, normal_inverse = {}, []

    def lower_row(i):
        for j in range(i + 1):
            entry = gram[i, j]
            for m in range(j):
                entry = entry - lower[i, m] * lower[j, m]
            if j < i:
                lower[i, j] = entry * upright[j]
            else:
                upright.append(lax.rsqrt(entry))
                lower[i, i] = entry * upright[i]

    def arnoldi(j):
        image = [SHIFT * entry for entry in coords[j - 1]] + [coords[j - 1][j - 1]]
        for m in range(1, j):
            image[m] = image[m] + coords[j - 1][m - 1]
        fresh = image
        for i in range(j):
            seen = image[i] * lower[i, i]
            for m in range(i + 1, j + 1):
                seen = seen + image[m] * lower[m, i]
            coeff = seen * lengths[i]
            hess[i, j - 1] = coeff
            fresh = [
                entry - coeff * coords[i][m] if m <= i else entry for m, entry in enumerate(fresh)
            ]
        length = image[j] * lower[j, j]
        square = length * length + epsilon
        scale = lax.rsqrt(square)
        hess[j, j - 1] = square * scale
        coords.append([entry * scale for entry in fresh])
        lengths.append(1.0 / (length * scale))
        entries = []
        for n in range(j):
            entry = None
            for i in range(n + 2):
                term = hess[i, j - 1] * hess[i, n]
                entry = term if entry is None else entry + term
            entries.append(entry)
        extend_factor(normal, normal_inverse, entries)

    collect(0, early, gram)
    for i in range(ITERS):
        lower_row(i)
    square = gram[0, 0] + epsilon
    scale = lax.rsqrt(square)
    beta = square * scale
    coords.append([scale])
    lengths.append(1.0 / (lower[0, 0] * scale))
    for j in range(1, ITERS):
        arnoldi(j)
    collect(1, late, gram)
    lower_row(ITERS)
    arnoldi(ITERS)

    packed = jnp.zeros((systems, lanes), f32)
    for (i, j), value in hess.items():
        packed = jnp.where(lane == i * ITERS + j, value, packed)
    turned = packed.T
    for i in range(ITERS + 1):
        hess_ref[i] = turned[i * ITERS : (i + 1) * ITERS, :]

    weights = factor_solve(normal, normal_inverse, [beta * hess[0, n] for n in range(ITERS)])
    mixed = []
    for m in range(ITERS):
        entry = None
        for i in range(m, ITERS):
            term = weights[i] * coords[i][m]
            entry = term if entry is None else entry + term
        mixed.append(entry)

    def combine(target, factors, b):
        for c in range(tile // lanes):
            out = None
            for m, factor in enumerate(factors):
                term = factor * krylov[m, :, pl.ds(b * tile + c * lanes, lanes)]
                out = term if out is None else out + term
            target[:, pl.ds(b * tile + c * lanes, lanes)] = out

    for b in range(block_rows):
        combine(last_ref, coords[ITERS], b)
        combine(solution_ref, mixed, b)

    finish_sends(ITERS)
    for g in range(2):
        for off in range(1, team):
            copy3(g, off, seat).wait_send()


def deliver(*refs):
    sources, targets, sem = refs[:3], refs[3:6], refs[6]
    copies = [
        pltpu.make_async_copy(source, target, sem.at[n])
        for n, (source, target) in enumerate(zip(sources, targets))
    ]
    for copy in copies:
        copy.start()
    for copy in copies:
        copy.wait()


def local(
    rows, cols, tile_values, block_columns, tile_counts, diagonal, sketch_rows, sketch_signs, right_side
):
    block_rows, slots, tile, _ = tile_values.shape
    span = 2 * block_rows + 1
    systems, width = right_side.shape
    scaling = 1.0 / math.sqrt(width * rows * cols)
    mates = 2 if rows % 2 == 0 else 1
    team = mates * cols
    chains = rows // mates
    share = SKETCH // team
    vectors = ITERS + 1
    vmem = pl.BlockSpec(memory_space=pltpu.VMEM)
    hbm = pl.BlockSpec(memory_space=pltpu.HBM)
    dma = pltpu.SemaphoreType.DMA
    found = pl.pallas_call(
        functools.partial(kernel, rows, cols, scaling),
        out_shape=(
            pltpu.VMEM((systems, width), f32),
            pltpu.VMEM((systems, width), f32),
            pltpu.VMEM((ITERS + 1, ITERS, systems), f32),
        ),
        in_specs=[hbm] * 7,
        out_specs=(vmem, vmem, vmem),
        scratch_shapes=[
            pltpu.SMEM(block_columns.shape, jnp.int32),
            pltpu.SMEM(tile_counts.shape, jnp.int32),
            pltpu.VMEM((1, width), f32),
            pltpu.VMEM((1, width), jnp.int32),
            pltpu.VMEM((1, width), jnp.int32),
            pltpu.VMEM((block_rows * slots + 1, tile, tile), bf16),
            pltpu.VMEM((block_rows * span, tile, tile), bf16),
            pltpu.SMEM((block_rows * span,), jnp.int32),
            pltpu.VMEM((width, SKETCH), bf16),
            pltpu.VMEM((vectors, systems, width), f32),
            pltpu.VMEM((ITERS, 3 * block_rows, 2 * systems, tile), bf16),
            pltpu.VMEM((vectors, team, systems, share), f32),
            pltpu.VMEM((vectors, team, systems, share), f32),
            pltpu.VMEM((vectors, chains, systems, share), f32),
            pltpu.VMEM((2, team, systems, 128), f32),
            dma((6,)),
            dma((block_rows,)),
            dma((ITERS, 2, 2)),
            dma((ITERS, 2, 2)),
            dma((vectors, team)),
            dma((vectors, team)),
            dma((vectors, chains - 1)),
            dma((vectors, chains - 1)),
            dma((2, team - 1)),
            dma((2, team - 1)),
        ],
        compiler_params=pltpu.CompilerParams(
            collective_id=0, has_side_effects=True, vmem_limit_bytes=67043328 - 160 * 1024
        ),
    )(
        block_columns,
        tile_counts,
        diagonal.reshape(1, width),
        sketch_rows.reshape(1, width),
        sketch_signs.reshape(1, width),
        right_side,
        tile_values,
    )
    iterate, last, hessenberg = pl.pallas_call(
        deliver,
        out_shape=[jax.ShapeDtypeStruct(ref.shape, f32) for ref in found],
        in_specs=[vmem] * 3,
        out_specs=[hbm] * 3,
        scratch_shapes=[dma((3,))],
    )(*[pltpu.with_memory_space_constraint(ref, pltpu.VMEM) for ref in found])
    return iterate, last, jnp.transpose(hessenberg, (2, 0, 1))


def solution(mesh):
    spec = P(("row", "col"))
    in_specs = (
        P(("row", "col"), None, None, None),
        P(("row", "col"), None),
        spec,
        spec,
        spec,
        spec,
        P(None, ("row", "col")),
    )
    out_specs = (P(None, ("row", "col")), P(None, ("row", "col")), P())
    body = functools.partial(local, mesh.shape["row"], mesh.shape["col"])
    return jax.shard_map(body, mesh=mesh, in_specs=in_specs, out_specs=out_specs, check_vma=False)
```

```python
import functools
import math

import jax
import jax.numpy as jnp
from jax import lax
from jax.experimental import pallas as pl
from jax.experimental.pallas import tpu as pltpu
from jax.sharding import PartitionSpec as P

SKETCH = 1024
ITERS = 4
SHIFT = 1.75
epsilon = 1e-06
MESH = pl.DeviceIdType.MESH
f32 = jnp.float32
bf16 = jnp.bfloat16


def split_parts(value):
    head = value.astype(bf16)
    return jnp.concatenate([head, (value - head.astype(f32)).astype(bf16)], axis=0)


def extend_factor(factor, inverse, entries):
    row = len(inverse)
    for column in range(row):
        entry = entries[column]
        for inner in range(column):
            entry = entry - factor[row, inner] * factor[column, inner]
        factor[row, column] = entry * inverse[column]
    diag_part = entries[row]
    for inner in range(row):
        diag_part = diag_part - factor[row, inner] * factor[row, inner]
    inverse.append(lax.rsqrt(diag_part))


def factor_solve(factor, inverse, target):
    order = len(target)
    forward = []
    for column in range(order):
        entry = target[column]
        for inner in range(column):
            entry = entry - factor[column, inner] * forward[inner]
        forward.append(entry * inverse[column])
    result = [None] * order
    for column in reversed(range(order)):
        entry = forward[column]
        for inner in range(column + 1, order):
            entry = entry - factor[inner, column] * result[inner]
        result[column] = entry * inverse[column]
    return result


def nn_dot(a, b):
    return lax.dot_general(a, b, (((1,), (0,)), ((), ())), preferred_element_type=f32)


def kernel(
    rows,
    cols,
    scaling,
    columns_hbm,
    counts_hbm,
    diag_hbm,
    rows_hbm,
    signs_hbm,
    right_hbm,
    tiles_hbm,
    solution_ref,
    last_ref,
    hess_ref,
    columns_ref,
    counts_ref,
    diag_ref,
    rows_ref,
    signs_ref,
    tiles,
    band,
    index_ref,
    projector,
    krylov,
    window,
    part,
    land1,
    land2,
    grams,
    load_sem,
    tile_sem,
    halo_send,
    halo_recv,
    send1,
    recv1,
    send2,
    recv2,
    send3,
    recv3,
):
    row = lax.axis_index("row")
    col = lax.axis_index("col")
    devices = rows * cols
    me = row * cols + col
    block_rows, slots, tile, _ = tiles_hbm.shape
    span = 2 * block_rows + 1
    systems, width = right_hbm.shape
    all_blocks = block_rows * devices
    share = land1.shape[-1]
    team = SKETCH // share
    mates = team // cols
    chains = rows // mates
    right = lax.rem(me + 1, devices)
    left = lax.rem(me + devices - 1, devices)
    right = (lax.div(right, cols), lax.rem(right, cols))
    left = (lax.div(left, cols), lax.rem(left, cols))
    chain = lax.div(row, mates)
    seat = lax.rem(row, mates) * cols + col

    def mate(number):
        return (chain * mates + lax.div(number, cols), lax.rem(number, cols))

    def link(number):
        return (number * mates + lax.rem(row, mates), col)

    parity = lax.rem(seat, 2)
    pair_to = [lax.rem(lax.div(seat, 2) + turn, team // 2) for turn in range(team // 2)]
    sides = [(turn, side) for turn in range(1, team // 2) for side in range(2)] + [(0, 1 - parity)]
    seat_to = [lax.rem(seat + off, team) for off in range(team)]
    seat_from = [lax.rem(seat + team - off, team) for off in range(team)]
    chain_to = [lax.rem(chain + off, chains) for off in range(chains)]
    chain_from = [lax.rem(chain + chains - off, chains) for off in range(chains)]

    right_load = pltpu.make_async_copy(right_hbm, krylov.at[0], load_sem.at[0])
    right_load.start()
    barrier = pltpu.get_barrier_semaphore()
    for peer in (left, right):
        pl.semaphore_signal(barrier, inc=1, device_id=peer, device_id_type=MESH)
    for number in chain_to[1:]:
        pl.semaphore_signal(barrier, inc=1, device_id=link(number), device_id_type=MESH)
    for number in seat_to[1:]:
        pl.semaphore_signal(barrier, inc=1, device_id=mate(number), device_id_type=MESH)

    loads = [
        pltpu.make_async_copy(source, target, load_sem.at[n + 1])
        for n, (source, target) in enumerate(
            [
                (rows_hbm, rows_ref),
                (signs_hbm, signs_ref),
                (columns_hbm, columns_ref),
                (counts_hbm, counts_ref),
                (diag_hbm, diag_ref),
            ]
        )
    ]
    tile_loads = [
        pltpu.make_async_copy(tiles_hbm.at[b], tiles.at[pl.ds(b * slots, slots)], tile_sem)
        for b in range(block_rows)
    ]
    for load in loads + tile_loads:
        load.start()
    tiles[block_rows * slots] = jnp.zeros((tile, tile), bf16)
    half = block_rows // 2
    lanes = 128

    def block_at(b):
        return pl.ds(b * tile, tile)

    def halo_copies(k, far):
        lower, upper = 0, block_rows - half
        starts = ((0, right, lower if far else upper), (2, left, upper if far else lower))
        return [
            pltpu.make_async_remote_copy(
                src_ref=window.at[k, pl.ds(block_rows + start, half)],
                dst_ref=window.at[k, pl.ds(side * block_rows + start, half)],
                send_sem=halo_send,
                recv_sem=halo_recv.at[k, far],
                device_id=peer,
                device_id_type=MESH,
            )
            for side, peer, start in starts
        ]

    def whole(ref, send_sem, recv_sem):
        return pltpu.make_async_remote_copy(
            src_ref=ref,
            dst_ref=ref,
            send_sem=send_sem,
            recv_sem=recv_sem,
            device_id=right,
            device_id_type=MESH,
        )

    def await_halo(k, far):
        whole(window.at[k, pl.ds(0, 2 * half)], halo_send, halo_recv.at[k, far]).wait_recv()

    def send_halo(k):
        for far in range(2):
            for copy in halo_copies(k, far):
                copy.start()

    def copy1(k, turn, side):
        return pltpu.make_async_remote_copy(
            src_ref=part.at[k, 2 * turn + side],
            dst_ref=land1.at[k, 2 * turn + parity],
            send_sem=send1,
            recv_sem=recv1.at[k],
            device_id=mate(2 * pair_to[turn] + side),
            device_id_type=MESH,
        )

    def copy2(k, off, source):
        return pltpu.make_async_remote_copy(
            src_ref=land2.at[k, source],
            dst_ref=land2.at[k, source],
            send_sem=send2,
            recv_sem=recv2.at[k],
            device_id=link(chain_to[off]),
            device_id_type=MESH,
        )

    def copy3(g, off, source):
        return pltpu.make_async_remote_copy(
            src_ref=grams.at[g, source],
            dst_ref=grams.at[g, source],
            send_sem=send3,
            recv_sem=recv3.at[g],
            device_id=mate(seat_to[off]),
            device_id_type=MESH,
        )

    right_load.wait()
    for b in range(block_rows):
        window[0, block_rows + b] = split_parts(krylov[0, :, block_at(b)])
    pl.semaphore_wait(barrier, team + chains)
    send_halo(0)

    for load in loads:
        load.wait()
    first = me * block_rows
    for b in range(block_rows):
        spots = []
        for slot in range(slots):
            spot = lax.rem(columns_ref[b, slot] - first - b + block_rows + all_blocks, all_blocks)
            spots.append(jnp.where(slot < counts_ref[b], spot, span))
        for d in range(span):
            chosen = block_rows * slots
            for slot in range(slots):
                chosen = jnp.where(spots[slot] == d, b * slots + slot, chosen)
            index_ref[b * span + d] = chosen

    for c in range(width // lanes):
        here = pl.ds(c * lanes, lanes)
        target = jnp.broadcast_to(rows_ref[0:1, here].astype(f32), (lanes, lanes)).T
        sign = jnp.broadcast_to((2 * signs_ref[0:1, here] - 1).astype(f32), (lanes, lanes)).T
        for m in range(SKETCH // lanes):
            spot = (lax.broadcasted_iota(jnp.int32, (lanes, lanes), 1) + m * lanes).astype(f32)
            projector[here, pl.ds(m * lanes, lanes)] = jnp.where(spot == target, sign, 0.0).astype(bf16)

    used = tiles.at[pl.ds(0, block_rows * slots)]
    pltpu.make_async_copy(used, used, tile_sem).wait()

    def turn(b, carry):
        for d in range(span):
            band[b * span + d] = tiles[index_ref[b * span + d]].T
        return carry

    lax.fori_loop(0, block_rows, turn, 0)

    def fold(total):
        return total[:systems] + total[systems:]

    def matvec(k, b, spots):
        total = None
        for spot in spots:
            if 0 <= spot - b < span:
                term = nn_dot(window[k, spot], band[b * span + spot - b])
                total = term if total is None else total + term
        return fold(total)

    spots = list(range(3 * block_rows))
    own = spots[block_rows : 2 * block_rows]
    near = spots[half:block_rows] + spots[2 * block_rows : 2 * block_rows + half]
    far = spots[:half] + spots[2 * block_rows + half :]

    def stage1(k, values):
        for turn in range(team // 2):
            here = pl.ds(pl.multiple_of(pair_to[turn] * 2 * share, 2 * share), 2 * share)
            total = None
            for b in range(block_rows):
                term = nn_dot(values[b], projector[block_at(b), here])
                total = term if total is None else total + term
            total = fold(total) * scaling
            for side in range(2):
                part[k, 2 * turn + side] = total[:, side * share : (side + 1) * share]
        for turn, side in sides:
            copy1(k, turn, side).start()

    def stage2(k):
        whole(land1.at[k, pl.ds(0, team - 1)], send1, recv1.at[k]).wait_recv()
        total = part[k, parity]
        for turn, side in sides:
            total = total + land1[k, 2 * turn + side]
        land2[k, chain] = total
        for off in range(1, chains):
            copy2(k, off, chain).start()

    def gathered(k):
        whole(land2.at[k, pl.ds(0, chains - 1)], send2, recv2.at[k]).wait_recv()
        total = land2[k, 0]
        for r in range(1, chains):
            total = total + land2[k, r]
        return total

    for k in range(ITERS):
        for b in range(block_rows):
            scaled = (diag_ref[0:1, block_at(b)] - SHIFT) * krylov[k, :, block_at(b)]
            krylov[k + 1, :, block_at(b)] = scaled + matvec(k, b, own)
        for m in range(0 if k == 1 else max(k, 1), k + 1):
            stage1(m, [window[m, block_rows + b] for b in range(block_rows)])
        for m in range(0 if k == 2 else max(k - 1, 1), k):
            stage2(m)
        await_halo(k, 0)
        for b in range(block_rows):
            krylov[k + 1, :, block_at(b)] += matvec(k, b, near)
        await_halo(k, 1)
        values = []
        for b in range(block_rows):
            fresh = krylov[k + 1, :, block_at(b)] + matvec(k, b, far)
            krylov[k + 1, :, block_at(b)] = fresh
            values.append(split_parts(fresh))
            if k + 1 < ITERS:
                window[k + 1, block_rows + b] = values[b]
        if k + 1 < ITERS:
            send_halo(k + 1)
    stage1(ITERS, values)
    stage2(ITERS - 1)

    lane = lax.broadcasted_iota(jnp.int32, (systems, lanes), 1)
    sketches = []

    def pair_sums(pairs):
        packed = jnp.zeros((systems, lanes), f32)
        for p, (i, j) in enumerate(pairs):
            value = jnp.sum(sketches[i] * sketches[j], axis=1, keepdims=True)
            packed = jnp.where(lane == p, value, packed)
        return packed

    def publish(g, packed):
        grams[g, seat] = packed
        for off in range(1, team):
            copy3(g, off, seat).start()

    def collect(g, pairs, gram):
        whole(grams.at[g, pl.ds(0, team - 1)], send3, recv3.at[g]).wait_recv()
        total = grams[g, 0]
        for c in range(1, team):
            total = total + grams[g, c]
        for p, pair in enumerate(pairs):
            gram[pair] = jnp.broadcast_to(total[:, p : p + 1], (systems, lanes))

    early = [(i, j) for i in range(ITERS) for j in range(i + 1)]
    late = [(ITERS, j) for j in range(ITERS + 1)]
    for k in range(ITERS - 1):
        sketches.append(gathered(k))
    stage2(ITERS)
    sketches.append(gathered(ITERS - 1))
    publish(0, pair_sums(early))
    sketches.append(gathered(ITERS))
    publish(1, pair_sums(late))

    gram = {}
    lower = {}
    upright = []
    coords = []
    lengths = []
    hess = {}
    normal, normal_inverse = {}, []

    def lower_row(i):
        for j in range(i + 1):
            entry = gram[i, j]
            for m in range(j):
                entry = entry - lower[i, m] * lower[j, m]
            if j < i:
                lower[i, j] = entry * upright[j]
            else:
                upright.append(lax.rsqrt(entry))
                lower[i, i] = entry * upright[i]

    def arnoldi(j):
        image = [SHIFT * entry for entry in coords[j - 1]] + [coords[j - 1][j - 1]]
        for m in range(1, j):
            image[m] = image[m] + coords[j - 1][m - 1]
        fresh = image
        for i in range(j):
            seen = image[i] * lower[i, i]
            for m in range(i + 1, j + 1):
                seen = seen + image[m] * lower[m, i]
            coeff = seen * lengths[i]
            hess[i, j - 1] = coeff
            fresh = [
                entry - coeff * coords[i][m] if m <= i else entry for m, entry in enumerate(fresh)
            ]
        length = image[j] * lower[j, j]
        square = length * length + epsilon
        scale = lax.rsqrt(square)
        hess[j, j - 1] = square * scale
        coords.append([entry * scale for entry in fresh])
        lengths.append(1.0 / (length * scale))
        entries = []
        for n in range(j):
            entry = None
            for i in range(n + 2):
                term = hess[i, j - 1] * hess[i, n]
                entry = term if entry is None else entry + term
            entries.append(entry)
        extend_factor(normal, normal_inverse, entries)

    collect(0, early, gram)
    for i in range(ITERS):
        lower_row(i)
    square = gram[0, 0] + epsilon
    scale = lax.rsqrt(square)
    beta = square * scale
    coords.append([scale])
    lengths.append(1.0 / (lower[0, 0] * scale))
    for j in range(1, ITERS):
        arnoldi(j)
    collect(1, late, gram)
    lower_row(ITERS)
    arnoldi(ITERS)

    packed = jnp.zeros((systems, lanes), f32)
    for (i, j), value in hess.items():
        packed = jnp.where(lane == i * ITERS + j, value, packed)
    turned = packed.T
    for i in range(ITERS + 1):
        hess_ref[i] = turned[i * ITERS : (i + 1) * ITERS, :]

    weights = factor_solve(normal, normal_inverse, [beta * hess[0, n] for n in range(ITERS)])
    mixed = []
    for m in range(ITERS):
        entry = None
        for i in range(m, ITERS):
            term = weights[i] * coords[i][m]
            entry = term if entry is None else entry + term
        mixed.append(entry)

    def combine(target, factors, b):
        for c in range(tile // lanes):
            out = None
            for m, factor in enumerate(factors):
                term = factor * krylov[m, :, pl.ds(b * tile + c * lanes, lanes)]
                out = term if out is None else out + term
            target[:, pl.ds(b * tile + c * lanes, lanes)] = out

    for b in range(block_rows):
        combine(last_ref, coords[ITERS], b)
        combine(solution_ref, mixed, b)

    whole(window.at[:, pl.ds(0, 2 * block_rows)], halo_send, halo_recv.at[0, 0]).wait_send()
    whole(part.at[:, pl.ds(0, team - 1)], send1, recv1.at[0]).wait_send()
    whole(land2.at[:, pl.ds(0, chains - 1)], send2, recv2.at[0]).wait_send()
    whole(grams.at[:, pl.ds(0, team - 1)], send3, recv3.at[0]).wait_send()


def deliver(*refs):
    sources, targets, sem = refs[:3], refs[3:6], refs[6]
    copies = [
        pltpu.make_async_copy(source, target, sem.at[n])
        for n, (source, target) in enumerate(zip(sources, targets))
    ]
    for copy in copies:
        copy.start()
    for copy in copies:
        copy.wait()


def local(
    rows, cols, tile_values, block_columns, tile_counts, diagonal, sketch_rows, sketch_signs, right_side
):
    block_rows, slots, tile, _ = tile_values.shape
    span = 2 * block_rows + 1
    systems, width = right_side.shape
    scaling = 1.0 / math.sqrt(width * rows * cols)
    mates = 2 if rows % 2 == 0 else 1
    team = mates * cols
    chains = rows // mates
    share = SKETCH // team
    vectors = ITERS + 1
    vmem = pl.BlockSpec(memory_space=pltpu.VMEM)
    hbm = pl.BlockSpec(memory_space=pltpu.HBM)
    dma = pltpu.SemaphoreType.DMA
    found = pl.pallas_call(
        functools.partial(kernel, rows, cols, scaling),
        out_shape=(
            pltpu.VMEM((systems, width), f32),
            pltpu.VMEM((systems, width), f32),
            pltpu.VMEM((ITERS + 1, ITERS, systems), f32),
        ),
        in_specs=[hbm] * 7,
        out_specs=(vmem, vmem, vmem),
        scratch_shapes=[
            pltpu.SMEM(block_columns.shape, jnp.int32),
            pltpu.SMEM(tile_counts.shape, jnp.int32),
            pltpu.VMEM((1, width), f32),
            pltpu.VMEM((1, width), jnp.int32),
            pltpu.VMEM((1, width), jnp.int32),
            pltpu.VMEM((block_rows * slots + 1, tile, tile), bf16),
            pltpu.VMEM((block_rows * span, tile, tile), bf16),
            pltpu.SMEM((block_rows * span,), jnp.int32),
            pltpu.VMEM((width, SKETCH), bf16),
            pltpu.VMEM((vectors, systems, width), f32),
            pltpu.VMEM((ITERS, 3 * block_rows, 2 * systems, tile), bf16),
            pltpu.VMEM((vectors, team, systems, share), f32),
            pltpu.VMEM((vectors, team, systems, share), f32),
            pltpu.VMEM((vectors, chains, systems, share), f32),
            pltpu.VMEM((2, team, systems, 128), f32),
            dma((6,)),
            dma,
            dma,
            dma((ITERS, 2)),
            dma,
            dma((vectors,)),
            dma,
            dma((vectors,)),
            dma,
            dma((2,)),
        ],
        compiler_params=pltpu.CompilerParams(
            collective_id=0, has_side_effects=True, vmem_limit_bytes=67043328 - 160 * 1024
        ),
    )(
        block_columns,
        tile_counts,
        diagonal.reshape(1, width),
        sketch_rows.reshape(1, width),
        sketch_signs.reshape(1, width),
        right_side,
        tile_values,
    )
    iterate, last, hessenberg = pl.pallas_call(
        deliver,
        out_shape=[jax.ShapeDtypeStruct(ref.shape, f32) for ref in found],
        in_specs=[vmem] * 3,
        out_specs=[hbm] * 3,
        scratch_shapes=[dma((3,))],
    )(*[pltpu.with_memory_space_constraint(ref, pltpu.VMEM) for ref in found])
    return iterate, last, jnp.transpose(hessenberg, (2, 0, 1))


def solution(mesh):
    spec = P(("row", "col"))
    in_specs = (
        P(("row", "col"), None, None, None),
        P(("row", "col"), None),
        spec,
        spec,
        spec,
        spec,
        P(None, ("row", "col")),
    )
    out_specs = (P(None, ("row", "col")), P(None, ("row", "col")), P())
    body = functools.partial(local, mesh.shape["row"], mesh.shape["col"])
    return jax.shard_map(body, mesh=mesh, in_specs=in_specs, out_specs=out_specs, check_vma=False)
```

```python
import functools
import math

import jax
import jax.numpy as jnp
from jax import lax
from jax.experimental import pallas as pl
from jax.experimental.pallas import tpu as pltpu
from jax.sharding import PartitionSpec as P

SKETCH = 1024
ITERS = 4
SHIFT = 1.75
epsilon = 1e-06
MESH = pl.DeviceIdType.MESH
f32 = jnp.float32
bf16 = jnp.bfloat16


def split_parts(value):
    head = value.astype(bf16)
    return jnp.concatenate([head, (value - head.astype(f32)).astype(bf16)], axis=0)


def extend_factor(factor, inverse, entries):
    row = len(inverse)
    for column in range(row):
        entry = entries[column]
        for inner in range(column):
            entry = entry - factor[row, inner] * factor[column, inner]
        factor[row, column] = entry * inverse[column]
    diag_part = entries[row]
    for inner in range(row):
        diag_part = diag_part - factor[row, inner] * factor[row, inner]
    inverse.append(lax.rsqrt(diag_part))


def factor_solve(factor, inverse, target):
    order = len(target)
    forward = []
    for column in range(order):
        entry = target[column]
        for inner in range(column):
            entry = entry - factor[column, inner] * forward[inner]
        forward.append(entry * inverse[column])
    result = [None] * order
    for column in reversed(range(order)):
        entry = forward[column]
        for inner in range(column + 1, order):
            entry = entry - factor[inner, column] * result[inner]
        result[column] = entry * inverse[column]
    return result


def nn_dot(a, b):
    return lax.dot_general(a, b, (((1,), (0,)), ((), ())), preferred_element_type=f32)


def kernel(
    rows,
    cols,
    scaling,
    columns_hbm,
    counts_hbm,
    diag_hbm,
    rows_hbm,
    signs_hbm,
    right_hbm,
    tiles_hbm,
    solution_ref,
    last_ref,
    hess_ref,
    columns_ref,
    counts_ref,
    diag_ref,
    rows_ref,
    signs_ref,
    tiles,
    band,
    index_ref,
    projector,
    krylov,
    window,
    part,
    land1,
    land2,
    grams,
    load_sem,
    tile_sem,
    halo_send,
    halo_recv,
    send1,
    recv1,
    send2,
    recv2,
    send3,
    recv3,
):
    row = lax.axis_index("row")
    col = lax.axis_index("col")
    devices = rows * cols
    me = row * cols + col
    block_rows, slots, tile, _ = tiles_hbm.shape
    span = 2 * block_rows + 1
    systems, width = right_hbm.shape
    all_blocks = block_rows * devices
    share = land1.shape[-1]
    team = SKETCH // share
    mates = team // cols
    chains = rows // mates
    right = lax.rem(me + 1, devices)
    left = lax.rem(me + devices - 1, devices)
    right = (lax.div(right, cols), lax.rem(right, cols))
    left = (lax.div(left, cols), lax.rem(left, cols))
    barrier = pltpu.get_barrier_semaphore()
    for peer in (left, right):
        pl.semaphore_signal(barrier, inc=1, device_id=peer, device_id_type=MESH)
    right_load = pltpu.make_async_copy(right_hbm, krylov.at[0], load_sem.at[0])
    right_load.start()
    chain = lax.div(row, mates)
    seat = lax.rem(row, mates) * cols + col

    def mate(number):
        return (chain * mates + lax.div(number, cols), lax.rem(number, cols))

    def link(number):
        return (number * mates + lax.rem(row, mates), col)

    parity = lax.rem(seat, 2)
    pair_to = [lax.rem(lax.div(seat, 2) + turn, team // 2) for turn in range(team // 2)]
    sides = [(turn, side) for turn in range(1, team // 2) for side in range(2)] + [(0, 1 - parity)]
    seat_to = [lax.rem(seat + off, team) for off in range(team)]
    chain_to = [lax.rem(chain + off, chains) for off in range(chains)]

    for number in chain_to[1:]:
        pl.semaphore_signal(barrier, inc=1, device_id=link(number), device_id_type=MESH)
    for number in seat_to[1:]:
        pl.semaphore_signal(barrier, inc=1, device_id=mate(number), device_id_type=MESH)
    loads = [
        pltpu.make_async_copy(source, target, load_sem.at[n + 1])
        for n, (source, target) in enumerate(
            [
                (rows_hbm, rows_ref),
                (signs_hbm, signs_ref),
                (columns_hbm, columns_ref),
                (counts_hbm, counts_ref),
                (diag_hbm, diag_ref),
            ]
        )
    ]
    tile_loads = [
        pltpu.make_async_copy(tiles_hbm.at[b], tiles.at[pl.ds(b * slots, slots)], tile_sem)
        for b in range(block_rows)
    ]
    for load in loads + tile_loads:
        load.start()
    tiles[block_rows * slots] = jnp.zeros((tile, tile), bf16)
    half = block_rows // 2
    lanes = 128

    def block_at(b):
        return pl.ds(b * tile, tile)

    def halo_copies(k, start):
        return [
            pltpu.make_async_remote_copy(
                src_ref=window.at[k, pl.ds(block_rows + start, half)],
                dst_ref=window.at[k, pl.ds(side * block_rows + start, half)],
                send_sem=halo_send,
                recv_sem=halo_recv.at[k, side // 2, start // half],
                device_id=peer,
                device_id_type=MESH,
            )
            for side, peer in ((0, right), (2, left))
        ]

    def whole(ref, send_sem, recv_sem):
        return pltpu.make_async_remote_copy(
            src_ref=ref,
            dst_ref=ref,
            send_sem=send_sem,
            recv_sem=recv_sem,
            device_id=right,
            device_id_type=MESH,
        )

    def await_halo(k, side, start):
        spots = pl.ds(2 * side * block_rows + start, half)
        whole(window.at[k, spots], halo_send, halo_recv.at[k, side, start // half]).wait_recv()

    def send_halo(k, start):
        for copy in halo_copies(k, start):
            copy.start()

    def copy1(k, turn, side):
        return pltpu.make_async_remote_copy(
            src_ref=part.at[k, 2 * turn + side],
            dst_ref=land1.at[k, 2 * turn + parity],
            send_sem=send1,
            recv_sem=recv1.at[k],
            device_id=mate(2 * pair_to[turn] + side),
            device_id_type=MESH,
        )

    def copy2(k, off, source):
        return pltpu.make_async_remote_copy(
            src_ref=land2.at[k, source],
            dst_ref=land2.at[k, source],
            send_sem=send2,
            recv_sem=recv2.at[k],
            device_id=link(chain_to[off]),
            device_id_type=MESH,
        )

    def copy3(g, off, source):
        return pltpu.make_async_remote_copy(
            src_ref=grams.at[g, source],
            dst_ref=grams.at[g, source],
            send_sem=send3,
            recv_sem=recv3.at[g],
            device_id=mate(seat_to[off]),
            device_id_type=MESH,
        )

    right_load.wait()
    for b in range(block_rows):
        window[0, block_rows + b] = split_parts(krylov[0, :, block_at(b)])
    pl.semaphore_wait(barrier, team + chains)
    send_halo(0, 0)
    send_halo(0, half)

    for load in loads:
        load.wait()
    first = me * block_rows
    for b in range(block_rows):
        spots = []
        for slot in range(slots):
            spot = lax.rem(columns_ref[b, slot] - first - b + block_rows + all_blocks, all_blocks)
            spots.append(jnp.where(slot < counts_ref[b], spot, span))
        for d in range(span):
            chosen = block_rows * slots
            for slot in range(slots):
                chosen = jnp.where(spots[slot] == d, b * slots + slot, chosen)
            index_ref[b * span + d] = chosen

    for c in range(width // lanes):
        here = pl.ds(c * lanes, lanes)
        target = jnp.broadcast_to(rows_ref[0:1, here].astype(f32), (lanes, lanes)).T
        sign = jnp.broadcast_to((2 * signs_ref[0:1, here] - 1).astype(f32), (lanes, lanes)).T
        for m in range(SKETCH // lanes):
            spot = (lax.broadcasted_iota(jnp.int32, (lanes, lanes), 1) + m * lanes).astype(f32)
            projector[here, pl.ds(m * lanes, lanes)] = jnp.where(spot == target, sign, 0.0).astype(bf16)

    used = tiles.at[pl.ds(0, block_rows * slots)]
    pltpu.make_async_copy(used, used, tile_sem).wait()

    def turn(b, carry):
        for d in range(span):
            band[b * span + d] = tiles[index_ref[b * span + d]].T
        return carry

    lax.fori_loop(0, block_rows, turn, 0)

    def fold(total):
        return total[:systems] + total[systems:]

    def matvec(k, b, spots):
        total = None
        for spot in spots:
            if 0 <= spot - b < span:
                term = nn_dot(window[k, spot], band[b * span + spot - b])
                total = term if total is None else total + term
        return fold(total)

    spots = list(range(3 * block_rows))
    own = spots[block_rows : 2 * block_rows]
    groups = ((0, range(half)), (half, range(half, block_rows)))

    def add(k, side, starts, wanted):
        for b in wanted:
            here = [
                spot
                for start in starts
                for spot in range(2 * side * block_rows + start, 2 * side * block_rows + start + half)
                if 0 <= spot - b < span
            ]
            if here:
                krylov[k + 1, :, block_at(b)] += matvec(k, b, here)

    def publish_rows(k, start, wanted):
        for b in wanted:
            window[k + 1, block_rows + b] = split_parts(krylov[k + 1, :, block_at(b)])
        if k + 1 < ITERS:
            send_halo(k + 1, start)

    def left_last(k):
        for start in (0, half):
            await_halo(k, 1, start)
        add(k, 1, (0, half), range(block_rows))
        await_halo(k, 0, 0)
        add(k, 0, (0,), range(block_rows))
        await_halo(k, 0, half)
        for start, wanted in groups:
            add(k, 0, (half,), wanted)
            publish_rows(k, start, wanted)

    def right_last(k):
        for start in (0, half):
            await_halo(k, 0, start)
        add(k, 0, (0, half), range(block_rows))
        await_halo(k, 1, 0)
        add(k, 1, (0,), range(half))
        publish_rows(k, 0, range(half))
        add(k, 1, (0,), range(half, block_rows))
        await_halo(k, 1, half)
        add(k, 1, (half,), range(half, block_rows))
        publish_rows(k, half, range(half, block_rows))

    def stage1(k, values):
        for turn in range(team // 2):
            here = pl.ds(pl.multiple_of(pair_to[turn] * 2 * share, 2 * share), 2 * share)
            total = None
            for b in range(block_rows):
                term = nn_dot(values[b], projector[block_at(b), here])
                total = term if total is None else total + term
            total = fold(total) * scaling
            for side in range(2):
                part[k, 2 * turn + side] = total[:, side * share : (side + 1) * share]
        for turn, side in sides:
            copy1(k, turn, side).start()

    def stage2(k):
        whole(land1.at[k, pl.ds(0, team - 1)], send1, recv1.at[k]).wait_recv()
        total = part[k, parity]
        for turn, side in sides:
            total = total + land1[k, 2 * turn + side]
        land2[k, chain] = total
        for off in range(1, chains):
            copy2(k, off, chain).start()

    def gathered(k):
        whole(land2.at[k, pl.ds(0, chains - 1)], send2, recv2.at[k]).wait_recv()
        total = land2[k, 0]
        for r in range(1, chains):
            total = total + land2[k, r]
        return total

    for k in range(ITERS):
        for b in range(block_rows):
            scaled = (diag_ref[0:1, block_at(b)] - SHIFT) * krylov[k, :, block_at(b)]
            krylov[k + 1, :, block_at(b)] = scaled + matvec(k, b, own)
        for m in range(0 if k == 1 else max(k, 1), k + 1):
            stage1(m, [window[m, block_rows + b] for b in range(block_rows)])
        for m in range(0 if k == 2 else max(k - 1, 1), k):
            stage2(m)
        pl.when(me < devices // 2)(functools.partial(left_last, k))
        pl.when(me >= devices // 2)(functools.partial(right_last, k))
    stage1(ITERS, [window[ITERS, block_rows + b] for b in range(block_rows)])
    stage2(ITERS - 1)

    lane = lax.broadcasted_iota(jnp.int32, (systems, lanes), 1)
    sketches = []

    def pair_sums(pairs):
        packed = jnp.zeros((systems, lanes), f32)
        for p, (i, j) in enumerate(pairs):
            value = jnp.sum(sketches[i] * sketches[j], axis=1, keepdims=True)
            packed = jnp.where(lane == p, value, packed)
        return packed

    def publish(g, packed):
        grams[g, seat] = packed
        for off in range(1, team):
            copy3(g, off, seat).start()

    def collect(g, pairs, gram):
        whole(grams.at[g, pl.ds(0, team - 1)], send3, recv3.at[g]).wait_recv()
        total = grams[g, 0]
        for c in range(1, team):
            total = total + grams[g, c]
        for p, pair in enumerate(pairs):
            gram[pair] = jnp.broadcast_to(total[:, p : p + 1], (systems, lanes))

    early = [(i, j) for i in range(ITERS) for j in range(i + 1)]
    late = [(ITERS, j) for j in range(ITERS + 1)]
    for k in range(ITERS - 1):
        sketches.append(gathered(k))
    stage2(ITERS)
    sketches.append(gathered(ITERS - 1))
    publish(0, pair_sums(early))
    sketches.append(gathered(ITERS))
    publish(1, pair_sums(late))

    gram = {}
    lower = {}
    upright = []
    coords = []
    lengths = []
    hess = {}
    normal, normal_inverse = {}, []

    def lower_row(i):
        for j in range(i + 1):
            entry = gram[i, j]
            for m in range(j):
                entry = entry - lower[i, m] * lower[j, m]
            if j < i:
                lower[i, j] = entry * upright[j]
            else:
                upright.append(lax.rsqrt(entry))
                lower[i, i] = entry * upright[i]

    def arnoldi(j):
        image = [SHIFT * entry for entry in coords[j - 1]] + [coords[j - 1][j - 1]]
        for m in range(1, j):
            image[m] = image[m] + coords[j - 1][m - 1]
        fresh = image
        for i in range(j):
            seen = image[i] * lower[i, i]
            for m in range(i + 1, j + 1):
                seen = seen + image[m] * lower[m, i]
            coeff = seen * lengths[i]
            hess[i, j - 1] = coeff
            fresh = [
                entry - coeff * coords[i][m] if m <= i else entry for m, entry in enumerate(fresh)
            ]
        length = image[j] * lower[j, j]
        square = length * length + epsilon
        scale = lax.rsqrt(square)
        hess[j, j - 1] = square * scale
        coords.append([entry * scale for entry in fresh])
        lengths.append(1.0 / (length * scale))
        entries = []
        for n in range(j):
            entry = None
            for i in range(n + 2):
                term = hess[i, j - 1] * hess[i, n]
                entry = term if entry is None else entry + term
            entries.append(entry)
        extend_factor(normal, normal_inverse, entries)

    collect(0, early, gram)
    for i in range(ITERS):
        lower_row(i)
    square = gram[0, 0] + epsilon
    scale = lax.rsqrt(square)
    beta = square * scale
    coords.append([scale])
    lengths.append(1.0 / (lower[0, 0] * scale))
    for j in range(1, ITERS):
        arnoldi(j)
    collect(1, late, gram)
    lower_row(ITERS)
    arnoldi(ITERS)

    packed = jnp.zeros((systems, lanes), f32)
    for (i, j), value in hess.items():
        packed = jnp.where(lane == i * ITERS + j, value, packed)
    turned = packed.T
    for i in range(ITERS + 1):
        hess_ref[i] = turned[i * ITERS : (i + 1) * ITERS, :]

    weights = factor_solve(normal, normal_inverse, [beta * hess[0, n] for n in range(ITERS)])
    mixed = []
    for m in range(ITERS):
        entry = None
        for i in range(m, ITERS):
            term = weights[i] * coords[i][m]
            entry = term if entry is None else entry + term
        mixed.append(entry)

    def combine(target, factors, b):
        for c in range(tile // lanes):
            out = None
            for m, factor in enumerate(factors):
                term = factor * krylov[m, :, pl.ds(b * tile + c * lanes, lanes)]
                out = term if out is None else out + term
            target[:, pl.ds(b * tile + c * lanes, lanes)] = out

    for b in range(block_rows):
        combine(last_ref, coords[ITERS], b)
        combine(solution_ref, mixed, b)

    sent = window.at[pl.ds(0, ITERS), pl.ds(0, 2 * block_rows)]
    whole(sent, halo_send, halo_recv.at[0, 0, 0]).wait_send()
    whole(part.at[:, pl.ds(0, team - 1)], send1, recv1.at[0]).wait_send()
    whole(land2.at[:, pl.ds(0, chains - 1)], send2, recv2.at[0]).wait_send()
    whole(grams.at[:, pl.ds(0, team - 1)], send3, recv3.at[0]).wait_send()


def deliver(*refs):
    sources, targets, sem = refs[:3], refs[3:6], refs[6]
    copies = [
        pltpu.make_async_copy(source, target, sem.at[n])
        for n, (source, target) in enumerate(zip(sources, targets))
    ]
    for copy in copies:
        copy.start()
    for copy in copies:
        copy.wait()


def local(
    rows, cols, tile_values, block_columns, tile_counts, diagonal, sketch_rows, sketch_signs, right_side
):
    block_rows, slots, tile, _ = tile_values.shape
    span = 2 * block_rows + 1
    systems, width = right_side.shape
    scaling = 1.0 / math.sqrt(width * rows * cols)
    mates = 2 if rows % 2 == 0 else 1
    team = mates * cols
    chains = rows // mates
    share = SKETCH // team
    vectors = ITERS + 1
    vmem = pl.BlockSpec(memory_space=pltpu.VMEM)
    hbm = pl.BlockSpec(memory_space=pltpu.HBM)
    dma = pltpu.SemaphoreType.DMA
    found = pl.pallas_call(
        functools.partial(kernel, rows, cols, scaling),
        out_shape=(
            pltpu.VMEM((systems, width), f32),
            pltpu.VMEM((systems, width), f32),
            pltpu.VMEM((ITERS + 1, ITERS, systems), f32),
        ),
        in_specs=[hbm] * 7,
        out_specs=(vmem, vmem, vmem),
        scratch_shapes=[
            pltpu.SMEM(block_columns.shape, jnp.int32),
            pltpu.SMEM(tile_counts.shape, jnp.int32),
            pltpu.VMEM((1, width), f32),
            pltpu.VMEM((1, width), jnp.int32),
            pltpu.VMEM((1, width), jnp.int32),
            pltpu.VMEM((block_rows * slots + 1, tile, tile), bf16),
            pltpu.VMEM((block_rows * span, tile, tile), bf16),
            pltpu.SMEM((block_rows * span,), jnp.int32),
            pltpu.VMEM((width, SKETCH), bf16),
            pltpu.VMEM((vectors, systems, width), f32),
            pltpu.VMEM((vectors, 3 * block_rows, 2 * systems, tile), bf16),
            pltpu.VMEM((vectors, team, systems, share), f32),
            pltpu.VMEM((vectors, team, systems, share), f32),
            pltpu.VMEM((vectors, chains, systems, share), f32),
            pltpu.VMEM((2, team, systems, 128), f32),
            dma((6,)),
            dma,
            dma,
            dma((ITERS, 2, 2)),
            dma,
            dma((vectors,)),
            dma,
            dma((vectors,)),
            dma,
            dma((2,)),
        ],
        compiler_params=pltpu.CompilerParams(
            collective_id=0, has_side_effects=True, vmem_limit_bytes=67043328 - 160 * 1024
        ),
    )(
        block_columns,
        tile_counts,
        diagonal.reshape(1, width),
        sketch_rows.reshape(1, width),
        sketch_signs.reshape(1, width),
        right_side,
        tile_values,
    )
    iterate, last, hessenberg = pl.pallas_call(
        deliver,
        out_shape=[jax.ShapeDtypeStruct(ref.shape, f32) for ref in found],
        in_specs=[vmem] * 3,
        out_specs=[hbm] * 3,
        scratch_shapes=[dma((3,))],
    )(*[pltpu.with_memory_space_constraint(ref, pltpu.VMEM) for ref in found])
    return iterate, last, jnp.transpose(hessenberg, (2, 0, 1))


def solution(mesh):
    spec = P(("row", "col"))
    in_specs = (
        P(("row", "col"), None, None, None),
        P(("row", "col"), None),
        spec,
        spec,
        spec,
        spec,
        P(None, ("row", "col")),
    )
    out_specs = (P(None, ("row", "col")), P(None, ("row", "col")), P())
    body = functools.partial(local, mesh.shape["row"], mesh.shape["col"])
    return jax.shard_map(body, mesh=mesh, in_specs=in_specs, out_specs=out_specs, check_vma=False)
```

```python
import functools
import math

import jax
import jax.numpy as jnp
from jax import lax
from jax.experimental import pallas as pl
from jax.experimental.pallas import tpu as pltpu
from jax.sharding import PartitionSpec as P

SKETCH = 1024
ITERS = 4
SHIFT = 1.75
epsilon = 1e-06
MESH = pl.DeviceIdType.MESH
f32 = jnp.float32
bf16 = jnp.bfloat16


def split_parts(value):
    head = value.astype(bf16)
    return jnp.concatenate([head, (value - head.astype(f32)).astype(bf16)], axis=0)


def extend_factor(factor, inverse, entries):
    row = len(inverse)
    for column in range(row):
        entry = entries[column]
        for inner in range(column):
            entry = entry - factor[row, inner] * factor[column, inner]
        factor[row, column] = entry * inverse[column]
    diag_part = entries[row]
    for inner in range(row):
        diag_part = diag_part - factor[row, inner] * factor[row, inner]
    inverse.append(lax.rsqrt(diag_part))


def factor_solve(factor, inverse, target):
    order = len(target)
    forward = []
    for column in range(order):
        entry = target[column]
        for inner in range(column):
            entry = entry - factor[column, inner] * forward[inner]
        forward.append(entry * inverse[column])
    result = [None] * order
    for column in reversed(range(order)):
        entry = forward[column]
        for inner in range(column + 1, order):
            entry = entry - factor[inner, column] * result[inner]
        result[column] = entry * inverse[column]
    return result


def nn_dot(a, b):
    return lax.dot_general(a, b, (((1,), (0,)), ((), ())), preferred_element_type=f32)


def kernel(
    rows,
    cols,
    scaling,
    columns_hbm,
    counts_hbm,
    diag_hbm,
    rows_hbm,
    signs_hbm,
    right_hbm,
    tiles_hbm,
    solution_ref,
    last_ref,
    hess_ref,
    columns_ref,
    counts_ref,
    diag_ref,
    rows_ref,
    signs_ref,
    tiles,
    band,
    index_ref,
    projector,
    krylov,
    window,
    part,
    land1,
    land2,
    direct,
    straight,
    grams,
    load_sem,
    tile_sem,
    halo_send,
    halo_recv,
    send1,
    recv1,
    send2,
    recv2,
    send3,
    recv3,
    send4,
    recv4,
):
    row = lax.axis_index("row")
    col = lax.axis_index("col")
    devices = rows * cols
    me = row * cols + col
    block_rows, slots, tile, _ = tiles_hbm.shape
    span = 2 * block_rows + 1
    systems, width = right_hbm.shape
    all_blocks = block_rows * devices
    share = land1.shape[-1]
    team = SKETCH // share
    mates = team // cols
    chains = rows // mates
    right = lax.rem(me + 1, devices)
    left = lax.rem(me + devices - 1, devices)
    right = (lax.div(right, cols), lax.rem(right, cols))
    left = (lax.div(left, cols), lax.rem(left, cols))
    barrier = pltpu.get_barrier_semaphore()
    for peer in (left, right):
        pl.semaphore_signal(barrier, inc=1, device_id=peer, device_id_type=MESH)
    right_load = pltpu.make_async_copy(right_hbm, krylov.at[0], load_sem.at[0])
    right_load.start()
    chain = lax.div(row, mates)
    seat = lax.rem(row, mates) * cols + col

    def mate(number):
        return (chain * mates + lax.div(number, cols), lax.rem(number, cols))

    def link(number):
        return (number * mates + lax.rem(row, mates), col)

    parity = lax.rem(seat, 2)
    pair_to = [lax.rem(lax.div(seat, 2) + turn, team // 2) for turn in range(team // 2)]
    sides = [(turn, side) for turn in range(1, team // 2) for side in range(2)] + [(0, 1 - parity)]
    seat_to = [lax.rem(seat + off, team) for off in range(team)]
    chain_to = [lax.rem(chain + off, chains) for off in range(chains)]

    for number in chain_to[1:]:
        pl.semaphore_signal(barrier, inc=1, device_id=link(number), device_id_type=MESH)
    for number in seat_to[1:]:
        pl.semaphore_signal(barrier, inc=1, device_id=mate(number), device_id_type=MESH)
    last = devices - 1
    trailing = jnp.logical_or(me == 0, me == last)
    loads = [
        pltpu.make_async_copy(source, target, load_sem.at[n + 1])
        for n, (source, target) in enumerate(
            [
                (rows_hbm, rows_ref),
                (signs_hbm, signs_ref),
                (columns_hbm, columns_ref),
                (counts_hbm, counts_ref),
                (diag_hbm, diag_ref),
            ]
        )
    ]
    tile_loads = [
        pltpu.make_async_copy(tiles_hbm.at[b], tiles.at[pl.ds(b * slots, slots)], tile_sem)
        for b in range(block_rows)
    ]
    for load in loads + tile_loads:
        load.start()
    part[ITERS] = jnp.zeros(part.shape[1:], f32)
    tiles[block_rows * slots] = jnp.zeros((tile, tile), bf16)
    half = block_rows // 2
    lanes = 128

    def block_at(b):
        return pl.ds(b * tile, tile)

    def halo_copies(k, start):
        return [
            pltpu.make_async_remote_copy(
                src_ref=window.at[k, pl.ds(block_rows + start, half)],
                dst_ref=window.at[k, pl.ds(side * block_rows + start, half)],
                send_sem=halo_send,
                recv_sem=halo_recv.at[k, side // 2, start // half],
                device_id=peer,
                device_id_type=MESH,
            )
            for side, peer in ((0, right), (2, left))
        ]

    def whole(ref, send_sem, recv_sem):
        return pltpu.make_async_remote_copy(
            src_ref=ref,
            dst_ref=ref,
            send_sem=send_sem,
            recv_sem=recv_sem,
            device_id=right,
            device_id_type=MESH,
        )

    def await_halo(k, side, start):
        spots = pl.ds(2 * side * block_rows + start, half)
        whole(window.at[k, spots], halo_send, halo_recv.at[k, side, start // half]).wait_recv()

    def send_halo(k, start):
        for copy in halo_copies(k, start):
            copy.start()

    def copy1(k, turn, side, source=None):
        return pltpu.make_async_remote_copy(
            src_ref=part.at[k, 2 * turn + side] if source is None else source,
            dst_ref=land1.at[k, 2 * turn + parity],
            send_sem=send1,
            recv_sem=recv1.at[k],
            device_id=mate(2 * pair_to[turn] + side),
            device_id_type=MESH,
        )

    def copy2(k, off, source):
        return pltpu.make_async_remote_copy(
            src_ref=land2.at[k, source],
            dst_ref=land2.at[k, source],
            send_sem=send2,
            recv_sem=recv2.at[k],
            device_id=link(chain_to[off]),
            device_id_type=MESH,
        )

    def copy3(g, off, source):
        return pltpu.make_async_remote_copy(
            src_ref=grams.at[g, source],
            dst_ref=grams.at[g, source],
            send_sem=send3,
            recv_sem=recv3.at[g],
            device_id=mate(seat_to[off]),
            device_id_type=MESH,
        )

    right_load.wait()
    for b in range(block_rows):
        window[0, block_rows + b] = split_parts(krylov[0, :, block_at(b)])
    pl.semaphore_wait(barrier, team + chains)
    send_halo(0, 0)
    send_halo(0, half)

    for load in loads:
        load.wait()
    first = me * block_rows
    for b in range(block_rows):
        spots = []
        for slot in range(slots):
            spot = lax.rem(columns_ref[b, slot] - first - b + block_rows + all_blocks, all_blocks)
            spots.append(jnp.where(slot < counts_ref[b], spot, span))
        for d in range(span):
            chosen = block_rows * slots
            for slot in range(slots):
                chosen = jnp.where(spots[slot] == d, b * slots + slot, chosen)
            index_ref[b * span + d] = chosen

    for c in range(width // lanes):
        here = pl.ds(c * lanes, lanes)
        target = jnp.broadcast_to(rows_ref[0:1, here].astype(f32), (lanes, lanes)).T
        sign = jnp.broadcast_to((2 * signs_ref[0:1, here] - 1).astype(f32), (lanes, lanes)).T
        for m in range(SKETCH // lanes):
            spot = (lax.broadcasted_iota(jnp.int32, (lanes, lanes), 1) + m * lanes).astype(f32)
            projector[here, pl.ds(m * lanes, lanes)] = jnp.where(spot == target, sign, 0.0).astype(bf16)

    used = tiles.at[pl.ds(0, block_rows * slots)]
    pltpu.make_async_copy(used, used, tile_sem).wait()

    def turn(b, carry):
        for d in range(span):
            band[b * span + d] = tiles[index_ref[b * span + d]].T
        return carry

    lax.fori_loop(0, block_rows, turn, 0)

    def fold(total):
        return total[:systems] + total[systems:]

    def matvec(k, b, spots):
        total = None
        for spot in spots:
            if 0 <= spot - b < span:
                term = nn_dot(window[k, spot], band[b * span + spot - b])
                total = term if total is None else total + term
        return fold(total)

    spots = list(range(3 * block_rows))
    last_chain = chains - 1
    own = spots[block_rows : 2 * block_rows]
    groups = ((0, range(half)), (half, range(half, block_rows)))

    def add(k, side, starts, wanted):
        for b in wanted:
            here = [
                spot
                for start in starts
                for spot in range(2 * side * block_rows + start, 2 * side * block_rows + start + half)
                if 0 <= spot - b < span
            ]
            if here:
                krylov[k + 1, :, block_at(b)] += matvec(k, b, here)

    def publish_rows(k, start, wanted):
        for b in wanted:
            window[k + 1, block_rows + b] = split_parts(krylov[k + 1, :, block_at(b)])
        if k + 1 < ITERS:
            send_halo(k + 1, start)

    def left_last(k):
        for start in (0, half):
            await_halo(k, 1, start)
        add(k, 1, (0, half), range(block_rows))
        await_halo(k, 0, 0)
        add(k, 0, (0,), range(block_rows))
        await_halo(k, 0, half)
        for start, wanted in groups:
            add(k, 0, (half,), wanted)
            publish_rows(k, start, wanted)

    def right_last(k):
        for start in (0, half):
            await_halo(k, 0, start)
        add(k, 0, (0, half), range(block_rows))
        await_halo(k, 1, 0)
        add(k, 1, (0,), range(half))
        publish_rows(k, 0, range(half))
        add(k, 1, (0,), range(half, block_rows))
        await_halo(k, 1, half)
        add(k, 1, (half,), range(half, block_rows))
        publish_rows(k, half, range(half, block_rows))

    def stage1(k, values):
        for turn in range(team // 2):
            here = pl.ds(pl.multiple_of(pair_to[turn] * 2 * share, 2 * share), 2 * share)
            total = None
            for b in range(block_rows):
                term = nn_dot(values[b], projector[block_at(b), here])
                total = term if total is None else total + term
            total = fold(total) * scaling
            for side in range(2):
                piece = total[:, side * share : (side + 1) * share]
                if k < ITERS:
                    part[k, 2 * turn + side] = piece
                else:
                    direct[2 * turn + side] = piece
        if k < ITERS:
            for turn, side in sides:
                copy1(k, turn, side).start()
        else:
            pl.when(trailing)(send_straight)
            pl.when(jnp.logical_not(trailing))(send_team)

    def copy4(chain_number, turn, side):
        number = 2 * pair_to[turn] + side
        end = jnp.where(me == 0, 0, 1)
        return pltpu.make_async_remote_copy(
            src_ref=direct.at[2 * turn + side],
            dst_ref=straight.at[end],
            send_sem=send4,
            recv_sem=recv4.at[end],
            device_id=(chain_number * mates + lax.div(number, cols), lax.rem(number, cols)),
            device_id_type=MESH,
        )

    def send_zeros():
        for turn, side in sides:
            copy1(ITERS, turn, side).start()

    def send_team():
        for turn, side in sides:
            copy1(ITERS, turn, side, direct.at[2 * turn + side]).start()

    def send_straight():
        for far in range(chains - 1):
            for turn in range(team // 2):
                for side in range(2):
                    copy4(jnp.where(me == 0, last_chain - far, far), turn, side).start()
        for turn, side in sides:
            copy4(chain, turn, side).start()
        straight[jnp.where(me == 0, 0, 1)] = direct[parity]

    def stage2(k):
        whole(land1.at[k, pl.ds(0, team - 1)], send1, recv1.at[k]).wait_recv()
        total = part[k, parity] if k < ITERS else jnp.where(trailing, 0.0, direct[parity])
        for turn, side in sides:
            total = total + land1[k, 2 * turn + side]
        land2[k, chain] = total
        for off in range(1, chains):
            copy2(k, off, chain).start()

    def gathered(k):
        whole(land2.at[k, pl.ds(0, chains - 1)], send2, recv2.at[k]).wait_recv()
        total = land2[k, 0]
        for r in range(1, chains):
            total = total + land2[k, r]
        if k == ITERS:
            for end in range(2):
                await_end = whole(straight.at[end], send4, recv4.at[end]).wait_recv
                pl.when(me != end * last)(await_end)
            total = total + straight[0] + straight[1]
        return total

    for k in range(ITERS):
        for b in range(block_rows):
            scaled = (diag_ref[0:1, block_at(b)] - SHIFT) * krylov[k, :, block_at(b)]
            krylov[k + 1, :, block_at(b)] = scaled + matvec(k, b, own)
        for m in range(0 if k == 1 else max(k, 1), k + 1):
            stage1(m, [window[m, block_rows + b] for b in range(block_rows)])
        for m in range(0 if k == 2 else max(k - 1, 1), k):
            stage2(m)
        if k == ITERS - 1:

            @pl.when(trailing)
            def _():
                send_zeros()
                stage2(ITERS - 1)

        pl.when(me < devices // 2)(functools.partial(left_last, k))
        pl.when(me >= devices // 2)(functools.partial(right_last, k))
    sketches = [gathered(0)]
    stage1(ITERS, [window[ITERS, block_rows + b] for b in range(block_rows)])
    pl.when(jnp.logical_not(trailing))(functools.partial(stage2, ITERS - 1))

    lane = lax.broadcasted_iota(jnp.int32, (systems, lanes), 1)
    def pair_sums(pairs):
        packed = jnp.zeros((systems, lanes), f32)
        for p, (i, j) in enumerate(pairs):
            value = jnp.sum(sketches[i] * sketches[j], axis=1, keepdims=True)
            packed = jnp.where(lane == p, value, packed)
        return packed

    def publish(g, packed):
        grams[g, seat] = packed
        for off in range(1, team):
            copy3(g, off, seat).start()

    def collect(g, pairs, gram):
        whole(grams.at[g, pl.ds(0, team - 1)], send3, recv3.at[g]).wait_recv()
        total = grams[g, 0]
        for c in range(1, team):
            total = total + grams[g, c]
        for p, pair in enumerate(pairs):
            gram[pair] = jnp.broadcast_to(total[:, p : p + 1], (systems, lanes))

    early = [(i, j) for i in range(ITERS) for j in range(i + 1)]
    late = [(ITERS, j) for j in range(ITERS + 1)]
    for k in range(1, ITERS - 1):
        sketches.append(gathered(k))
    stage2(ITERS)
    sketches.append(gathered(ITERS - 1))
    publish(0, pair_sums(early))
    sketches.append(gathered(ITERS))
    publish(1, pair_sums(late))

    gram = {}
    lower = {}
    upright = []
    coords = []
    lengths = []
    hess = {}
    normal, normal_inverse = {}, []

    def lower_row(i):
        for j in range(i + 1):
            entry = gram[i, j]
            for m in range(j):
                entry = entry - lower[i, m] * lower[j, m]
            if j < i:
                lower[i, j] = entry * upright[j]
            else:
                upright.append(lax.rsqrt(entry))
                lower[i, i] = entry * upright[i]

    def arnoldi(j):
        image = [SHIFT * entry for entry in coords[j - 1]] + [coords[j - 1][j - 1]]
        for m in range(1, j):
            image[m] = image[m] + coords[j - 1][m - 1]
        fresh = image
        for i in range(j):
            seen = image[i] * lower[i, i]
            for m in range(i + 1, j + 1):
                seen = seen + image[m] * lower[m, i]
            coeff = seen * lengths[i]
            hess[i, j - 1] = coeff
            fresh = [
                entry - coeff * coords[i][m] if m <= i else entry for m, entry in enumerate(fresh)
            ]
        length = image[j] * lower[j, j]
        square = length * length + epsilon
        scale = lax.rsqrt(square)
        hess[j, j - 1] = square * scale
        coords.append([entry * scale for entry in fresh])
        lengths.append(1.0 / (length * scale))
        entries = []
        for n in range(j):
            entry = None
            for i in range(n + 2):
                term = hess[i, j - 1] * hess[i, n]
                entry = term if entry is None else entry + term
            entries.append(entry)
        extend_factor(normal, normal_inverse, entries)

    collect(0, early, gram)
    for i in range(ITERS):
        lower_row(i)
    square = gram[0, 0] + epsilon
    scale = lax.rsqrt(square)
    beta = square * scale
    coords.append([scale])
    lengths.append(1.0 / (lower[0, 0] * scale))
    for j in range(1, ITERS):
        arnoldi(j)
    collect(1, late, gram)
    lower_row(ITERS)
    arnoldi(ITERS)

    packed = jnp.zeros((systems, lanes), f32)
    for (i, j), value in hess.items():
        packed = jnp.where(lane == i * ITERS + j, value, packed)
    turned = packed.T
    for i in range(ITERS + 1):
        hess_ref[i] = turned[i * ITERS : (i + 1) * ITERS, :]

    weights = factor_solve(normal, normal_inverse, [beta * hess[0, n] for n in range(ITERS)])
    mixed = []
    for m in range(ITERS):
        entry = None
        for i in range(m, ITERS):
            term = weights[i] * coords[i][m]
            entry = term if entry is None else entry + term
        mixed.append(entry)

    def combine(target, factors, b):
        for c in range(tile // lanes):
            out = None
            for m, factor in enumerate(factors):
                term = factor * krylov[m, :, pl.ds(b * tile + c * lanes, lanes)]
                out = term if out is None else out + term
            target[:, pl.ds(b * tile + c * lanes, lanes)] = out

    for b in range(block_rows):
        combine(last_ref, coords[ITERS], b)
        combine(solution_ref, mixed, b)

    sent = window.at[pl.ds(0, ITERS), pl.ds(0, 2 * block_rows)]
    whole(sent, halo_send, halo_recv.at[0, 0, 0]).wait_send()
    whole(part.at[:, pl.ds(0, team - 1)], send1, recv1.at[0]).wait_send()
    whole(land2.at[:, pl.ds(0, chains - 1)], send2, recv2.at[0]).wait_send()
    whole(grams.at[:, pl.ds(0, team - 1)], send3, recv3.at[0]).wait_send()
    pl.when(trailing)(whole(direct.at[pl.ds(0, last)], send4, recv4.at[0]).wait_send)


def deliver(*refs):
    sources, targets, sem = refs[:3], refs[3:6], refs[6]
    copies = [
        pltpu.make_async_copy(source, target, sem.at[n])
        for n, (source, target) in enumerate(zip(sources, targets))
    ]
    for copy in copies:
        copy.start()
    for copy in copies:
        copy.wait()


def local(
    rows, cols, tile_values, block_columns, tile_counts, diagonal, sketch_rows, sketch_signs, right_side
):
    block_rows, slots, tile, _ = tile_values.shape
    span = 2 * block_rows + 1
    systems, width = right_side.shape
    scaling = 1.0 / math.sqrt(width * rows * cols)
    mates = 2 if rows % 2 == 0 else 1
    team = mates * cols
    chains = rows // mates
    share = SKETCH // team
    vectors = ITERS + 1
    vmem = pl.BlockSpec(memory_space=pltpu.VMEM)
    hbm = pl.BlockSpec(memory_space=pltpu.HBM)
    dma = pltpu.SemaphoreType.DMA
    found = pl.pallas_call(
        functools.partial(kernel, rows, cols, scaling),
        out_shape=(
            pltpu.VMEM((systems, width), f32),
            pltpu.VMEM((systems, width), f32),
            pltpu.VMEM((ITERS + 1, ITERS, systems), f32),
        ),
        in_specs=[hbm] * 7,
        out_specs=(vmem, vmem, vmem),
        scratch_shapes=[
            pltpu.SMEM(block_columns.shape, jnp.int32),
            pltpu.SMEM(tile_counts.shape, jnp.int32),
            pltpu.VMEM((1, width), f32),
            pltpu.VMEM((1, width), jnp.int32),
            pltpu.VMEM((1, width), jnp.int32),
            pltpu.VMEM((block_rows * slots + 1, tile, tile), bf16),
            pltpu.VMEM((block_rows * span, tile, tile), bf16),
            pltpu.SMEM((block_rows * span,), jnp.int32),
            pltpu.VMEM((width, SKETCH), bf16),
            pltpu.VMEM((vectors, systems, width), f32),
            pltpu.VMEM((vectors, 3 * block_rows, 2 * systems, tile), bf16),
            pltpu.VMEM((vectors, team, systems, share), f32),
            pltpu.VMEM((vectors, team, systems, share), f32),
            pltpu.VMEM((vectors, chains, systems, share), f32),
            pltpu.VMEM((rows * cols, systems, share), f32),
            pltpu.VMEM((2, systems, share), f32),
            pltpu.VMEM((2, team, systems, 128), f32),
            dma((6,)),
            dma,
            dma,
            dma((ITERS, 2, 2)),
            dma,
            dma((vectors,)),
            dma,
            dma((vectors,)),
            dma,
            dma((2,)),
            dma,
            dma((2,)),
        ],
        compiler_params=pltpu.CompilerParams(
            collective_id=0, has_side_effects=True, vmem_limit_bytes=67043328 - 160 * 1024
        ),
    )(
        block_columns,
        tile_counts,
        diagonal.reshape(1, width),
        sketch_rows.reshape(1, width),
        sketch_signs.reshape(1, width),
        right_side,
        tile_values,
    )
    iterate, last, hessenberg = pl.pallas_call(
        deliver,
        out_shape=[jax.ShapeDtypeStruct(ref.shape, f32) for ref in found],
        in_specs=[vmem] * 3,
        out_specs=[hbm] * 3,
        scratch_shapes=[dma((3,))],
    )(*[pltpu.with_memory_space_constraint(ref, pltpu.VMEM) for ref in found])
    return iterate, last, jnp.transpose(hessenberg, (2, 0, 1))


def solution(mesh):
    spec = P(("row", "col"))
    in_specs = (
        P(("row", "col"), None, None, None),
        P(("row", "col"), None),
        spec,
        spec,
        spec,
        spec,
        P(None, ("row", "col")),
    )
    out_specs = (P(None, ("row", "col")), P(None, ("row", "col")), P())
    body = functools.partial(local, mesh.shape["row"], mesh.shape["col"])
    return jax.shard_map(body, mesh=mesh, in_specs=in_specs, out_specs=out_specs, check_vma=False)
```

```python
import functools
import math

import jax
import jax.numpy as jnp
from jax import lax
from jax.experimental import pallas as pl
from jax.experimental.pallas import tpu as pltpu
from jax.sharding import PartitionSpec as P

SKETCH = 1024
ITERS = 4
SHIFT = 1.75
epsilon = 1e-06
MESH = pl.DeviceIdType.MESH
f32 = jnp.float32
bf16 = jnp.bfloat16


def split_parts(value):
    head = value.astype(bf16)
    return jnp.concatenate([head, (value - head.astype(f32)).astype(bf16)], axis=0)


def extend_factor(factor, inverse, entries):
    row = len(inverse)
    for column in range(row):
        entry = entries[column]
        for inner in range(column):
            entry = entry - factor[row, inner] * factor[column, inner]
        factor[row, column] = entry * inverse[column]
    diag_part = entries[row]
    for inner in range(row):
        diag_part = diag_part - factor[row, inner] * factor[row, inner]
    inverse.append(lax.rsqrt(diag_part))


def factor_solve(factor, inverse, target):
    order = len(target)
    forward = []
    for column in range(order):
        entry = target[column]
        for inner in range(column):
            entry = entry - factor[column, inner] * forward[inner]
        forward.append(entry * inverse[column])
    result = [None] * order
    for column in reversed(range(order)):
        entry = forward[column]
        for inner in range(column + 1, order):
            entry = entry - factor[inner, column] * result[inner]
        result[column] = entry * inverse[column]
    return result


def nn_dot(a, b):
    return lax.dot_general(a, b, (((1,), (0,)), ((), ())), preferred_element_type=f32)


def kernel(
    rows,
    cols,
    scaling,
    columns_hbm,
    counts_hbm,
    diag_hbm,
    rows_hbm,
    signs_hbm,
    right_hbm,
    tiles_hbm,
    solution_ref,
    last_ref,
    hess_ref,
    columns_ref,
    counts_ref,
    diag_ref,
    rows_ref,
    signs_ref,
    tiles,
    band,
    index_ref,
    projector,
    krylov,
    window,
    part,
    land1,
    land2,
    direct,
    straight,
    grams,
    load_sem,
    tile_sem,
    halo_send,
    halo_recv,
    send1,
    recv1,
    send2,
    recv2,
    send3,
    recv3,
    send4,
    recv4,
):
    row = lax.axis_index("row")
    col = lax.axis_index("col")
    devices = rows * cols
    me = row * cols + col
    block_rows, slots, tile, _ = tiles_hbm.shape
    span = 2 * block_rows + 1
    systems, width = right_hbm.shape
    all_blocks = block_rows * devices
    share = land1.shape[-1]
    team = SKETCH // share
    mates = team // cols
    chains = rows // mates
    right = lax.rem(me + 1, devices)
    left = lax.rem(me + devices - 1, devices)
    right = (lax.div(right, cols), lax.rem(right, cols))
    left = (lax.div(left, cols), lax.rem(left, cols))
    barrier = pltpu.get_barrier_semaphore()
    for peer in (left, right):
        pl.semaphore_signal(barrier, inc=1, device_id=peer, device_id_type=MESH)
    right_load = pltpu.make_async_copy(right_hbm, krylov.at[0], load_sem.at[0])
    right_load.start()
    chain = lax.div(row, mates)
    seat = lax.rem(row, mates) * cols + col

    def mate(number):
        return (chain * mates + lax.div(number, cols), lax.rem(number, cols))

    def link(number):
        return (number * mates + lax.rem(row, mates), col)

    parity = lax.rem(seat, 2)
    pair_to = [lax.rem(lax.div(seat, 2) + turn, team // 2) for turn in range(team // 2)]
    sides = [(turn, side) for turn in range(1, team // 2) for side in range(2)] + [(0, 1 - parity)]
    seat_to = [lax.rem(seat + off, team) for off in range(team)]
    chain_to = [lax.rem(chain + off, chains) for off in range(chains)]

    for number in chain_to[1:]:
        pl.semaphore_signal(barrier, inc=1, device_id=link(number), device_id_type=MESH)
    for number in seat_to[1:]:
        pl.semaphore_signal(barrier, inc=1, device_id=mate(number), device_id_type=MESH)
    last = devices - 1
    trailing = jnp.logical_or(me == 0, me == last)
    loads = [
        pltpu.make_async_copy(source, target, load_sem.at[n + 1])
        for n, (source, target) in enumerate(
            [
                (rows_hbm, rows_ref),
                (signs_hbm, signs_ref),
                (columns_hbm, columns_ref),
                (counts_hbm, counts_ref),
                (diag_hbm, diag_ref),
            ]
        )
    ]
    tile_loads = [
        pltpu.make_async_copy(tiles_hbm.at[b], tiles.at[pl.ds(b * slots, slots)], tile_sem)
        for b in range(block_rows)
    ]
    for load in loads + tile_loads:
        load.start()
    part[ITERS] = jnp.zeros(part.shape[1:], f32)
    tiles[block_rows * slots] = jnp.zeros((tile, tile), bf16)
    half = block_rows // 2
    lanes = 128

    def block_at(b):
        return pl.ds(b * tile, tile)

    def halo_copies(k, start):
        return [
            pltpu.make_async_remote_copy(
                src_ref=window.at[k, pl.ds(block_rows + start, half)],
                dst_ref=window.at[k, pl.ds(side * block_rows + start, half)],
                send_sem=halo_send,
                recv_sem=halo_recv.at[k, side // 2, start // half],
                device_id=peer,
                device_id_type=MESH,
            )
            for side, peer in ((0, right), (2, left))
        ]

    def whole(ref, send_sem, recv_sem):
        return pltpu.make_async_remote_copy(
            src_ref=ref,
            dst_ref=ref,
            send_sem=send_sem,
            recv_sem=recv_sem,
            device_id=right,
            device_id_type=MESH,
        )

    def await_halo(k, side, start):
        spots = pl.ds(2 * side * block_rows + start, half)
        whole(window.at[k, spots], halo_send, halo_recv.at[k, side, start // half]).wait_recv()

    def send_halo(k, start):
        for copy in halo_copies(k, start):
            copy.start()

    def copy1(k, turn, side, source=None):
        return pltpu.make_async_remote_copy(
            src_ref=part.at[k, 2 * turn + side] if source is None else source,
            dst_ref=land1.at[k, 2 * turn + parity],
            send_sem=send1,
            recv_sem=recv1.at[k],
            device_id=mate(2 * pair_to[turn] + side),
            device_id_type=MESH,
        )

    def copy2(k, off, source):
        return pltpu.make_async_remote_copy(
            src_ref=land2.at[k, source],
            dst_ref=land2.at[k, source],
            send_sem=send2,
            recv_sem=recv2.at[k],
            device_id=link(chain_to[off]),
            device_id_type=MESH,
        )

    def copy3(g, off, source):
        return pltpu.make_async_remote_copy(
            src_ref=grams.at[g, source],
            dst_ref=grams.at[g, source],
            send_sem=send3,
            recv_sem=recv3.at[g],
            device_id=mate(seat_to[off]),
            device_id_type=MESH,
        )

    right_load.wait()
    for b in range(block_rows):
        window[0, block_rows + b] = split_parts(krylov[0, :, block_at(b)])
    pl.semaphore_wait(barrier, team + chains)
    send_halo(0, 0)
    send_halo(0, half)

    for load in loads:
        load.wait()
    first = me * block_rows
    for b in range(block_rows):
        spots = []
        for slot in range(slots):
            spot = lax.rem(columns_ref[b, slot] - first - b + block_rows + all_blocks, all_blocks)
            spots.append(jnp.where(slot < counts_ref[b], spot, span))
        for d in range(span):
            chosen = block_rows * slots
            for slot in range(slots):
                chosen = jnp.where(spots[slot] == d, b * slots + slot, chosen)
            index_ref[b * span + d] = chosen

    for c in range(width // lanes):
        here = pl.ds(c * lanes, lanes)
        target = jnp.broadcast_to(rows_ref[0:1, here].astype(f32), (lanes, lanes)).T
        sign = jnp.broadcast_to((2 * signs_ref[0:1, here] - 1).astype(f32), (lanes, lanes)).T
        for m in range(SKETCH // lanes):
            spot = (lax.broadcasted_iota(jnp.int32, (lanes, lanes), 1) + m * lanes).astype(f32)
            projector[here, pl.ds(m * lanes, lanes)] = jnp.where(spot == target, sign, 0.0).astype(bf16)

    used = tiles.at[pl.ds(0, block_rows * slots)]
    pltpu.make_async_copy(used, used, tile_sem).wait()

    def turn(b, carry):
        for d in range(span):
            band[b * span + d] = tiles[index_ref[b * span + d]].T
        return carry

    lax.fori_loop(0, block_rows, turn, 0)

    def fold(total):
        return total[:systems] + total[systems:]

    def matvec(k, b, spots):
        total = None
        for spot in spots:
            if 0 <= spot - b < span:
                term = nn_dot(window[k, spot], band[b * span + spot - b])
                total = term if total is None else total + term
        return fold(total)

    spots = list(range(3 * block_rows))
    own = spots[block_rows : 2 * block_rows]
    groups = ((0, range(half)), (half, range(half, block_rows)))

    def add(k, side, starts, wanted):
        for b in wanted:
            here = [
                spot
                for start in starts
                for spot in range(2 * side * block_rows + start, 2 * side * block_rows + start + half)
                if 0 <= spot - b < span
            ]
            if here:
                krylov[k + 1, :, block_at(b)] += matvec(k, b, here)

    def publish_rows(k, start, wanted):
        for b in wanted:
            window[k + 1, block_rows + b] = split_parts(krylov[k + 1, :, block_at(b)])
        if k + 1 < ITERS:
            send_halo(k + 1, start)

    def left_last(k):
        for start in (0, half):
            await_halo(k, 1, start)
        add(k, 1, (0, half), range(block_rows))
        await_halo(k, 0, 0)
        add(k, 0, (0,), range(block_rows))
        await_halo(k, 0, half)
        for start, wanted in groups:
            add(k, 0, (half,), wanted)
            publish_rows(k, start, wanted)

    def right_last(k):
        for start in (0, half):
            await_halo(k, 0, start)
        add(k, 0, (0, half), range(block_rows))
        await_halo(k, 1, 0)
        add(k, 1, (0,), range(half))
        publish_rows(k, 0, range(half))
        add(k, 1, (0,), range(half, block_rows))
        await_halo(k, 1, half)
        add(k, 1, (half,), range(half, block_rows))
        publish_rows(k, half, range(half, block_rows))

    def stage1(k, values):
        for turn in range(team // 2):
            here = pl.ds(pl.multiple_of(pair_to[turn] * 2 * share, 2 * share), 2 * share)
            total = None
            for b in range(block_rows):
                term = nn_dot(values[b], projector[block_at(b), here])
                total = term if total is None else total + term
            total = fold(total) * scaling
            for side in range(2):
                piece = total[:, side * share : (side + 1) * share]
                if k < ITERS:
                    part[k, 2 * turn + side] = piece
                else:
                    direct[2 * turn + side] = piece
        if k < ITERS:
            for turn, side in sides:
                copy1(k, turn, side).start()
        else:
            pl.when(me == 0)(functools.partial(send_straight, range(1, chains), True))
            pl.when(me == last)(functools.partial(send_straight, range(chains - 1), False))
            pl.when(jnp.logical_not(trailing))(send_team)

    def copy4(chain_number, turn, side):
        number = 2 * pair_to[turn] + side
        end = jnp.where(me == 0, 0, 1)
        return pltpu.make_async_remote_copy(
            src_ref=direct.at[2 * turn + side],
            dst_ref=straight.at[end],
            send_sem=send4,
            recv_sem=recv4.at[end],
            device_id=(chain_number * mates + lax.div(number, cols), lax.rem(number, cols)),
            device_id_type=MESH,
        )

    def send_zeros():
        for turn, side in sides:
            copy1(ITERS, turn, side).start()

    def send_team():
        for turn, side in sides:
            copy1(ITERS, turn, side, direct.at[2 * turn + side]).start()

    def send_straight(others, own_first):
        order = [(number, (turn, side)) for number in others for turn in range(team // 2) for side in range(2)]
        mine = [(chain, seat_of) for seat_of in sides]
        for number, (turn, side) in mine + order if own_first else order + mine:
            copy4(number, turn, side).start()
        straight[0 if own_first else 1] = direct[parity]

    def stage2(k):
        whole(land1.at[k, pl.ds(0, team - 1)], send1, recv1.at[k]).wait_recv()
        total = part[k, parity] if k < ITERS else jnp.where(trailing, 0.0, direct[parity])
        for turn, side in sides:
            total = total + land1[k, 2 * turn + side]
        land2[k, chain] = total
        for off in range(1, chains):
            copy2(k, off, chain).start()

    def gathered(k):
        whole(land2.at[k, pl.ds(0, chains - 1)], send2, recv2.at[k]).wait_recv()
        total = land2[k, 0]
        for r in range(1, chains):
            total = total + land2[k, r]
        if k == ITERS:
            for end in range(2):
                await_end = whole(straight.at[end], send4, recv4.at[end]).wait_recv
                pl.when(me != end * last)(await_end)
            total = total + straight[0] + straight[1]
        return total

    for k in range(ITERS):
        for b in range(block_rows):
            scaled = (diag_ref[0:1, block_at(b)] - SHIFT) * krylov[k, :, block_at(b)]
            krylov[k + 1, :, block_at(b)] = scaled + matvec(k, b, own)
        for m in range(0 if k == 1 else max(k, 1), k + 1):
            stage1(m, [window[m, block_rows + b] for b in range(block_rows)])
        for m in range(0 if k == 2 else max(k - 1, 1), k):
            stage2(m)
        if k == ITERS - 1:

            sketches = [gathered(0)]

            @pl.when(trailing)
            def _():
                send_zeros()
                stage2(ITERS - 1)

        pl.when(me < devices // 2)(functools.partial(left_last, k))
        pl.when(me >= devices // 2)(functools.partial(right_last, k))
    stage1(ITERS, [window[ITERS, block_rows + b] for b in range(block_rows)])
    pl.when(jnp.logical_not(trailing))(functools.partial(stage2, ITERS - 1))

    lane = lax.broadcasted_iota(jnp.int32, (systems, lanes), 1)
    def pair_sums(pairs):
        packed = jnp.zeros((systems, lanes), f32)
        for p, (i, j) in enumerate(pairs):
            value = jnp.sum(sketches[i] * sketches[j], axis=1, keepdims=True)
            packed = jnp.where(lane == p, value, packed)
        return packed

    def publish(g, packed):
        grams[g, seat] = packed
        for off in range(1, team):
            copy3(g, off, seat).start()

    def collect(g, pairs, gram):
        whole(grams.at[g, pl.ds(0, team - 1)], send3, recv3.at[g]).wait_recv()
        total = grams[g, 0]
        for c in range(1, team):
            total = total + grams[g, c]
        for p, pair in enumerate(pairs):
            gram[pair] = jnp.broadcast_to(total[:, p : p + 1], (systems, lanes))

    early = [(i, j) for i in range(ITERS) for j in range(i + 1)]
    late = [(ITERS, j) for j in range(ITERS + 1)]
    for k in range(1, ITERS - 1):
        sketches.append(gathered(k))
    stage2(ITERS)
    sketches.append(gathered(ITERS - 1))
    publish(0, pair_sums(early))
    sketches.append(gathered(ITERS))
    publish(1, pair_sums(late))

    gram = {}
    lower = {}
    upright = []
    coords = []
    lengths = []
    hess = {}
    normal, normal_inverse = {}, []

    def lower_row(i):
        for j in range(i + 1):
            entry = gram[i, j]
            for m in range(j):
                entry = entry - lower[i, m] * lower[j, m]
            if j < i:
                lower[i, j] = entry * upright[j]
            else:
                upright.append(lax.rsqrt(entry))
                lower[i, i] = entry * upright[i]

    def arnoldi(j):
        image = [SHIFT * entry for entry in coords[j - 1]] + [coords[j - 1][j - 1]]
        for m in range(1, j):
            image[m] = image[m] + coords[j - 1][m - 1]
        fresh = image
        for i in range(j):
            seen = image[i] * lower[i, i]
            for m in range(i + 1, j + 1):
                seen = seen + image[m] * lower[m, i]
            coeff = seen * lengths[i]
            hess[i, j - 1] = coeff
            fresh = [
                entry - coeff * coords[i][m] if m <= i else entry for m, entry in enumerate(fresh)
            ]
        length = image[j] * lower[j, j]
        square = length * length + epsilon
        scale = lax.rsqrt(square)
        hess[j, j - 1] = square * scale
        coords.append([entry * scale for entry in fresh])
        lengths.append(1.0 / (length * scale))
        entries = []
        for n in range(j):
            entry = None
            for i in range(n + 2):
                term = hess[i, j - 1] * hess[i, n]
                entry = term if entry is None else entry + term
            entries.append(entry)
        extend_factor(normal, normal_inverse, entries)

    collect(0, early, gram)
    for i in range(ITERS):
        lower_row(i)
    square = gram[0, 0] + epsilon
    scale = lax.rsqrt(square)
    beta = square * scale
    coords.append([scale])
    lengths.append(1.0 / (lower[0, 0] * scale))
    for j in range(1, ITERS):
        arnoldi(j)
    collect(1, late, gram)
    lower_row(ITERS)
    arnoldi(ITERS)

    packed = jnp.zeros((systems, lanes), f32)
    for (i, j), value in hess.items():
        packed = jnp.where(lane == i * ITERS + j, value, packed)
    turned = packed.T
    for i in range(ITERS + 1):
        hess_ref[i] = turned[i * ITERS : (i + 1) * ITERS, :]

    weights = factor_solve(normal, normal_inverse, [beta * hess[0, n] for n in range(ITERS)])
    mixed = []
    for m in range(ITERS):
        entry = None
        for i in range(m, ITERS):
            term = weights[i] * coords[i][m]
            entry = term if entry is None else entry + term
        mixed.append(entry)

    def combine(target, factors, b):
        for c in range(tile // lanes):
            out = None
            for m, factor in enumerate(factors):
                term = factor * krylov[m, :, pl.ds(b * tile + c * lanes, lanes)]
                out = term if out is None else out + term
            target[:, pl.ds(b * tile + c * lanes, lanes)] = out

    for b in range(block_rows):
        combine(last_ref, coords[ITERS], b)
        combine(solution_ref, mixed, b)

    sent = window.at[pl.ds(0, ITERS), pl.ds(0, 2 * block_rows)]
    whole(sent, halo_send, halo_recv.at[0, 0, 0]).wait_send()
    whole(part.at[:, pl.ds(0, team - 1)], send1, recv1.at[0]).wait_send()
    whole(land2.at[:, pl.ds(0, chains - 1)], send2, recv2.at[0]).wait_send()
    whole(grams.at[:, pl.ds(0, team - 1)], send3, recv3.at[0]).wait_send()
    pl.when(trailing)(whole(direct.at[pl.ds(0, last)], send4, recv4.at[0]).wait_send)


def deliver(*refs):
    sources, targets, sem = refs[:3], refs[3:6], refs[6]
    copies = [
        pltpu.make_async_copy(source, target, sem.at[n])
        for n, (source, target) in enumerate(zip(sources, targets))
    ]
    for copy in copies:
        copy.start()
    for copy in copies:
        copy.wait()


def local(
    rows, cols, tile_values, block_columns, tile_counts, diagonal, sketch_rows, sketch_signs, right_side
):
    block_rows, slots, tile, _ = tile_values.shape
    span = 2 * block_rows + 1
    systems, width = right_side.shape
    scaling = 1.0 / math.sqrt(width * rows * cols)
    mates = 2 if rows % 2 == 0 else 1
    team = mates * cols
    chains = rows // mates
    share = SKETCH // team
    vectors = ITERS + 1
    vmem = pl.BlockSpec(memory_space=pltpu.VMEM)
    hbm = pl.BlockSpec(memory_space=pltpu.HBM)
    dma = pltpu.SemaphoreType.DMA
    found = pl.pallas_call(
        functools.partial(kernel, rows, cols, scaling),
        out_shape=(
            pltpu.VMEM((systems, width), f32),
            pltpu.VMEM((systems, width), f32),
            pltpu.VMEM((ITERS + 1, ITERS, systems), f32),
        ),
        in_specs=[hbm] * 7,
        out_specs=(vmem, vmem, vmem),
        scratch_shapes=[
            pltpu.SMEM(block_columns.shape, jnp.int32),
            pltpu.SMEM(tile_counts.shape, jnp.int32),
            pltpu.VMEM((1, width), f32),
            pltpu.VMEM((1, width), jnp.int32),
            pltpu.VMEM((1, width), jnp.int32),
            pltpu.VMEM((block_rows * slots + 1, tile, tile), bf16),
            pltpu.VMEM((block_rows * span, tile, tile), bf16),
            pltpu.SMEM((block_rows * span,), jnp.int32),
            pltpu.VMEM((width, SKETCH), bf16),
            pltpu.VMEM((vectors, systems, width), f32),
            pltpu.VMEM((vectors, 3 * block_rows, 2 * systems, tile), bf16),
            pltpu.VMEM((vectors, team, systems, share), f32),
            pltpu.VMEM((vectors, team, systems, share), f32),
            pltpu.VMEM((vectors, chains, systems, share), f32),
            pltpu.VMEM((rows * cols, systems, share), f32),
            pltpu.VMEM((2, systems, share), f32),
            pltpu.VMEM((2, team, systems, 128), f32),
            dma((6,)),
            dma,
            dma,
            dma((ITERS, 2, 2)),
            dma,
            dma((vectors,)),
            dma,
            dma((vectors,)),
            dma,
            dma((2,)),
            dma,
            dma((2,)),
        ],
        compiler_params=pltpu.CompilerParams(
            collective_id=0, has_side_effects=True, vmem_limit_bytes=67043328 - 160 * 1024
        ),
    )(
        block_columns,
        tile_counts,
        diagonal.reshape(1, width),
        sketch_rows.reshape(1, width),
        sketch_signs.reshape(1, width),
        right_side,
        tile_values,
    )
    iterate, last, hessenberg = pl.pallas_call(
        deliver,
        out_shape=[jax.ShapeDtypeStruct(ref.shape, f32) for ref in found],
        in_specs=[vmem] * 3,
        out_specs=[hbm] * 3,
        scratch_shapes=[dma((3,))],
    )(*[pltpu.with_memory_space_constraint(ref, pltpu.VMEM) for ref in found])
    return iterate, last, jnp.transpose(hessenberg, (2, 0, 1))


def solution(mesh):
    spec = P(("row", "col"))
    in_specs = (
        P(("row", "col"), None, None, None),
        P(("row", "col"), None),
        spec,
        spec,
        spec,
        spec,
        P(None, ("row", "col")),
    )
    out_specs = (P(None, ("row", "col")), P(None, ("row", "col")), P())
    body = functools.partial(local, mesh.shape["row"], mesh.shape["col"])
    return jax.shard_map(body, mesh=mesh, in_specs=in_specs, out_specs=out_specs, check_vma=False)
```
